256 devices in a mesh: row: 32 (over x, z), col: 4 (over y_hi, core), ch: 2 (over y_lo).
Axes of the slice: x: 4, y: 4 (y_hi: 2, y_lo: 2; y = y_hi * 2 + y_lo), z: 8, core: 2. Of those that a mesh axis runs over, the one named last changes fastest.
Arguments:
- image_tokens: bfloat16 [512, 1024, 128], P(('row', 'ch'), 'col'), may hold values from -61 to 61
- labels: int32 [512, 1024], P(('row', 'ch'), 'col'), may hold values from 0 to 2
- rel_index: int32 [64, 64], replicated, may hold values from 0 to 224
- norm_gain: float32 [2, 2, 128], replicated, may hold values from 0.25 to 1.75
- norm_shift: float32 [2, 2, 128], replicated, may hold values from -1.5 to 1.5
- qkv_weight: bfloat16 [2, 3, 128, 128], P(None, None, None, 'ch'), may hold values from -5 to 5
- qkv_bias: float32 [2, 3, 128], P(None, None, 'ch'), may hold values from -1.5 to 1.5
- bias_table: float32 [2, 225, 4], P(None, None, 'ch'), may hold values from -4 to 4
- proj_weight: bfloat16 [2, 128, 128], P(None, 'ch'), may hold values from -0.5 to 0.5
- proj_bias: float32 [2, 128], replicated, may hold values from -1.5 to 1.5
- fc1_weight: bfloat16 [2, 128, 512], P(None, None, 'ch'), may hold values from -0.5 to 0.5
- fc1_bias: float32 [2, 512], P(None, 'ch'), may hold values from -2.5 to 2.5
- fc2_weight: bfloat16 [2, 512, 128], P(None, 'ch'), may hold values from -0.25 to 0.25
- fc2_bias: float32 [2, 128], replicated, may hold values from -1.5 to 1.5
Outputs:
- encoded: bfloat16 [512, 1024, 128], P(('row', 'ch'), 'col')
The draws below stay inside these ranges and needn't reach their ends.
All inputs are finite; a program needn't handle non-finite values.
Results may differ from the reference program's by a relative error of at most 0.014.
Values may be sent and summed in bfloat16 or wider, within the bound.
A program may use at most 128 MiB of HBM per device.

```python
import jax
import jax.numpy as jnp
from jax import lax

C = 128
HEADS = 4
MLP_WIDTH = 512
WIN = 8
SHIFT = 4
TABLE = 225
BLOCKS = 2
KINDS = 3
IMG_ROWS = 512
IMG_COLS = 1024


def draw_image_tokens(key, part):
    base_key = jax.random.fold_in(key, 11)
    values = jnp.clip(jax.random.normal(base_key, (IMG_ROWS, IMG_COLS, C), jnp.float32), -6.0, 6.0)
    return values.astype(jnp.bfloat16)


def draw_qkv_weight(key, part):
    noise_key = jax.random.fold_in(key, 21)
    noise = jnp.clip(jax.random.normal(noise_key, (BLOCKS, 3, C, C), jnp.float32), -4.0, 4.0) * C ** (-0.5)
    return noise.astype(jnp.bfloat16)


def place_ends(values, rng, smallest, high):
    dims = values.shape
    spot = [jax.random.randint(jax.random.fold_in(rng, axis), (), 0, dims[axis]) for axis in range(len(dims))]
    values = values.at[tuple(spot)].set(smallest)
    longest = dims.index(max(dims))
    spot[longest] = (spot[longest] + 1) % dims[longest]
    return values.at[tuple(spot)].set(high)


def steps_of(own_key, extent, shards, low, top_value):
    loudness = 1.0
    for dim, shards_of in shards:
        draws = jax.random.uniform(jax.random.fold_in(jax.random.fold_in(own_key, 6), dim), (shards_of,), jnp.float32, low / len(shards), top_value / len(shards))
        loudness = loudness * jnp.repeat(jnp.exp(draws), extent[dim] // shards_of).reshape((-1,) + (1,) * (len(extent) - 1 - dim))
    return loudness


def scatter_about(rng, extent, scale, bound, shards=(), held_as=jnp.bfloat16):
    drawn = scale * jax.random.normal(rng, extent, jnp.float32)
    if shards:
        drawn = drawn * steps_of(rng, extent, shards, -0.22, 0.18)
    return jnp.clip(drawn, -bound, bound).astype(held_as)


def setup_inputs(seed: int = 0) -> dict:
    arg_keys = jax.random.split(jax.random.key(seed), 15)
    image_tokens = draw_image_tokens(jax.random.fold_in(arg_keys[14], 71), 0)
    labels = place_ends(jax.random.randint(arg_keys[1], (IMG_ROWS, IMG_COLS), 0, KINDS), jax.random.fold_in(arg_keys[1], 1), 0, KINDS - 1).astype(jnp.int32)
    rel_index = place_ends(jax.random.randint(arg_keys[2], (WIN * WIN, WIN * WIN), 0, TABLE), jax.random.fold_in(arg_keys[2], 1), 0, TABLE - 1).astype(jnp.int32)
    norm_gain = jnp.clip(1.0 + 0.15 * jax.random.normal(arg_keys[3], (BLOCKS, 2, C), jnp.float32), 0.25, 1.75)
    norm_shift = scatter_about(arg_keys[4], (BLOCKS, 2, C), 0.3, 1.5, (), jnp.float32)
    qkv_weight = draw_qkv_weight(jax.random.fold_in(arg_keys[14], 71), 0)
    qkv_bias = scatter_about(arg_keys[6], (BLOCKS, 3, C), 0.3, 1.5, ((2, 2),), jnp.float32)
    bias_table = scatter_about(arg_keys[7], (BLOCKS, TABLE, HEADS), 1.0, 4.0, ((2, 2),), jnp.float32)
    proj_weight = scatter_about(arg_keys[8], (BLOCKS, C, C), C ** -0.5, 0.5, ((1, 2),))
    proj_bias = scatter_about(arg_keys[9], (BLOCKS, C), 0.3, 1.5, (), jnp.float32)
    fc1_weight = scatter_about(arg_keys[10], (BLOCKS, C, MLP_WIDTH), C ** -0.5, 0.5, ((2, 2),))
    fc1_bias = scatter_about(arg_keys[11], (BLOCKS, MLP_WIDTH), 0.5, 2.5, ((1, 2),), jnp.float32)
    fc2_weight = scatter_about(arg_keys[12], (BLOCKS, MLP_WIDTH, C), MLP_WIDTH ** -0.5, 0.25, ((1, 2),))
    fc2_bias = scatter_about(arg_keys[13], (BLOCKS, C), 0.3, 1.5, (), jnp.float32)
    return {"image_tokens": image_tokens, "labels": labels, "rel_index": rel_index, "norm_gain": norm_gain, "norm_shift": norm_shift, "qkv_weight": qkv_weight, "qkv_bias": qkv_bias, "bias_table": bias_table, "proj_weight": proj_weight, "proj_bias": proj_bias, "fc1_weight": fc1_weight, "fc1_bias": fc1_bias, "fc2_weight": fc2_weight, "fc2_bias": fc2_bias}


EPS = 1e-05

def layer_norm(values, gain, offset):
    widened = values.astype(jnp.float32)
    center = widened - lax.optimization_barrier(jnp.mean(widened, axis=-1, keepdims=True))
    spread = lax.optimization_barrier(jnp.mean(center * center, axis=-1, keepdims=True))
    return (center * lax.rsqrt(spread + EPS) * gain + offset).astype(jnp.bfloat16)

def position_bias(rel_index, table):
    entries = table.shape[0]
    onehot = (rel_index.reshape(-1, 1) == jnp.arange(entries, dtype=jnp.int32)[None, :]).astype(jnp.float32)
    picked = jnp.dot(onehot, table, precision=lax.Precision.HIGHEST, preferred_element_type=jnp.float32)
    length = rel_index.shape[0]
    return picked.T.reshape(table.shape[1], length, length)

def window_attention(triple, region, bias):
    rows, cols = (triple.shape[0], triple.shape[1])
    width = triple.shape[3]
    heads = bias.shape[0]
    depth = width // heads
    across = rows // WIN
    along = cols // WIN
    grid = triple.reshape(across, WIN, along, WIN, 3, heads, depth)
    grid = grid.transpose(0, 2, 4, 5, 1, 3, 6).reshape(across, along, 3, heads, WIN * WIN, depth)
    grid = grid.astype(jnp.float32)
    scores = jnp.einsum('abhpd,abhqd->abhpq', grid[:, :, 0], grid[:, :, 1])
    scores = scores * depth ** (-0.5) + bias
    if region is not None:
        window_ids = region.reshape(across, WIN, along, WIN).transpose(0, 2, 1, 3).reshape(across, along, WIN * WIN)
        allowed = window_ids[:, :, :, None] == window_ids[:, :, None, :]
        scores = jnp.where(allowed[:, :, None], scores, -jnp.inf)
    highest = lax.optimization_barrier(jnp.max(scores, axis=-1, keepdims=True))
    raised = jnp.exp(scores - highest)
    weights = (raised / lax.optimization_barrier(jnp.sum(raised, axis=-1, keepdims=True))).astype(jnp.bfloat16)
    mixed = jnp.einsum('abhpq,abhqd->abhpd', weights.astype(jnp.float32), grid[:, :, 2])
    mixed = mixed.astype(jnp.bfloat16).reshape(across, along, heads, WIN, WIN, depth)
    return mixed.transpose(0, 3, 1, 4, 2, 5).reshape(rows, cols, width)

def attend_image(triple, region, bias, offset):
    rolled = jnp.roll(triple, (-offset, -offset), axis=(0, 1))
    bands = rolled.reshape(IMG_ROWS // WIN, WIN, IMG_COLS, 3, C)
    if region is None:
        result = lax.map(lambda band: window_attention(band, None, bias), bands)
    else:
        region_bands = jnp.roll(region, (-offset, -offset), axis=(0, 1)).reshape(IMG_ROWS // WIN, WIN, IMG_COLS)
        result = lax.map(lambda pair: window_attention(pair[0], pair[1], bias), (bands, region_bands))
    result = result.reshape(IMG_ROWS, IMG_COLS, C)
    return jnp.roll(result, (offset, offset), axis=(0, 1))

def swin_block(tokens, block, region, offset, norm_gain, norm_shift, qkv_weight, qkv_bias, bias_table, proj_weight, proj_bias, fc1_weight, fc1_bias, fc2_weight, fc2_bias, rel_index):
    normed = layer_norm(tokens, norm_gain[block, 0], norm_shift[block, 0])
    stacked = qkv_weight[block].transpose(1, 0, 2).reshape(C, 3 * C)
    triple = jnp.dot(normed.reshape(-1, C), stacked, preferred_element_type=jnp.float32)
    triple = (triple.reshape(IMG_ROWS, IMG_COLS, 3, C) + qkv_bias[block]).astype(jnp.bfloat16)
    bias = position_bias(rel_index, bias_table[block])
    attended = attend_image(triple, region, bias, offset)
    mixed = jnp.dot(attended.reshape(-1, C), proj_weight[block], preferred_element_type=jnp.float32)
    middle = (tokens.astype(jnp.float32) + mixed.reshape(IMG_ROWS, IMG_COLS, C) + proj_bias[block]).astype(jnp.bfloat16)

    def feed(band):
        normed_two = layer_norm(band, norm_gain[block, 1], norm_shift[block, 1])
        inner = jnp.dot(normed_two.reshape(-1, C), fc1_weight[block], preferred_element_type=jnp.float32)
        hidden = jax.nn.gelu(inner + fc1_bias[block], approximate=False).astype(jnp.bfloat16)
        outer = jnp.dot(hidden, fc2_weight[block], preferred_element_type=jnp.float32).reshape(band.shape)
        return (band.astype(jnp.float32) + outer + fc2_bias[block]).astype(jnp.bfloat16)
    result = lax.map(feed, middle.reshape(IMG_ROWS // WIN, WIN, IMG_COLS, C))
    return result.reshape(IMG_ROWS, IMG_COLS, C)

def reference(image_tokens, labels, rel_index, norm_gain, norm_shift, qkv_weight, qkv_bias, bias_table, proj_weight, proj_bias, fc1_weight, fc1_bias, fc2_weight, fc2_bias):
    grid_rows = jnp.arange(IMG_ROWS, dtype=jnp.int32)
    grid_cols = jnp.arange(IMG_COLS, dtype=jnp.int32)
    region = labels * 4 + (grid_rows < SHIFT).astype(jnp.int32)[:, None] * 2 + (grid_cols < SHIFT).astype(jnp.int32)[None, :]
    current = image_tokens
    for block in range(BLOCKS):
        if block % 2 == 1:
            current = swin_block(current, block, region, SHIFT, norm_gain, norm_shift, qkv_weight, qkv_bias, bias_table, proj_weight, proj_bias, fc1_weight, fc1_bias, fc2_weight, fc2_bias, rel_index)
        else:
            current = swin_block(current, block, None, 0, norm_gain, norm_shift, qkv_weight, qkv_bias, bias_table, proj_weight, proj_bias, fc1_weight, fc1_bias, fc2_weight, fc2_bias, rel_index)
    return current
```

```python
import functools
import math

import jax
import jax.numpy as jnp
from jax import lax
from jax.experimental import pallas as pl
from jax.experimental.pallas import tpu as pltpu
from jax.sharding import PartitionSpec as P

WIN = 8
SHIFT = 4
HEADS = 4
EPS = 1e-05
C = 128
HEAD = 32
BF = jnp.bfloat16
F32 = jnp.float32
LOG2E = math.log2(math.e)
QSCALE = LOG2E / math.sqrt(HEAD)
ROOT_HALF = math.sqrt(0.5)
EXCLUDED = -1e30
MESH = pl.DeviceIdType.MESH

GROUP = 8
CHUNK = GROUP * WIN


def norm(x, gain, shift):
    center = x - jnp.mean(x, axis=-1, keepdims=True)
    spread = jnp.mean(center * center, axis=-1, keepdims=True)
    return (center * lax.rsqrt(spread + EPS) * gain + shift).astype(BF)


def dot(a, b):
    return jnp.dot(a, b, preferred_element_type=F32)


def side_by_side(a, b):
    return jnp.concatenate([a.astype(F32), b.astype(F32)], axis=1)


def kernel(
    x_ref, lab_ref, rel_ref, gain_ref, shift_ref, qkvw_ref, qkvb_ref, tbl_ref, projw_ref,
    projb_ref, fc1w_ref, fc1b_ref, fc2w_ref, fc2b_ref,
    out_ref,
    y, ids, wqkv, bqkv, wproj, wturned, bias,
    qk_s, qk_r, v_s, v_r, qkvb_r, tbl_r, fc1b_r, fc1w_r, fc2w_r,
    lab_up, lab_side, lab_diag,
    halo_s, halo_r, side_s, side_r, diag_r,
    att_own, att_s, att_r, att_side, att_diag,
    send, recv,
):
    cols = x_ref.shape[1]
    chunks = cols // CHUNK
    wins = cols // WIN
    groups = lax.axis_size("ch")
    bands = lax.axis_size("row") * groups
    tiles = lax.axis_size("col")
    ch = lax.axis_index("ch")
    col = lax.axis_index("col")
    band = lax.axis_index("row") * groups + ch

    def device(band_step, col_step):
        b = lax.rem(band + bands + band_step, bands)
        c = lax.rem(col + tiles + col_step, tiles)
        return {"row": b // groups, "col": c, "ch": lax.rem(b, groups)}

    partner = {"row": lax.axis_index("row"), "col": col, "ch": 1 - ch}
    up, down = device(-1, 0), device(1, 0)
    left, right = device(0, -1), device(0, 1)
    up_left, down_right = device(-1, -1), device(1, 1)

    barrier = pltpu.get_barrier_semaphore()
    peers = (up, down, left, right, up_left, down_right)
    for peer in peers:
        pl.semaphore_signal(barrier, inc=1, device_id=peer, device_id_type=MESH)

    for b in range(2):
        qk_s[b] = side_by_side(qkvw_ref[b, 0], qkvw_ref[b, 1]).astype(BF)
    v_s[...] = side_by_side(qkvw_ref[0, 2], qkvw_ref[1, 2]).astype(BF)

    pl.semaphore_wait(barrier, len(peers))

    def copy(i, src, dst, to):
        return pltpu.make_async_remote_copy(
            src_ref=src, dst_ref=dst, send_sem=send.at[i], recv_sem=recv.at[i],
            device_id=to, device_id_type=MESH,
        )

    def weight_copies(b):
        return [
            copy(4 + 8 * b, projw_ref.at[b], wproj.at[b, pl.ds(64, 64)], partner),
            copy(5 + 8 * b, fc1w_ref.at[b], fc1w_r.at[b], partner),
            copy(6 + 8 * b, fc2w_ref.at[b], fc2w_r.at[b], partner),
        ]

    first = [
        copy(0, qk_s.at[0], qk_r.at[0], partner),
        copy(1, v_s, v_r, partner),
        copy(2, qkvb_ref, qkvb_r, partner),
        copy(3, tbl_ref, tbl_r, partner),
        copy(7, fc1b_ref, fc1b_r, partner),
    ]
    second = [copy(8, qk_s.at[1], qk_r.at[1], partner)]
    weights = [weight_copies(0), weight_copies(1)]
    label_copies = [
        copy(9, lab_ref, lab_up, up),
        copy(10, lab_ref, lab_side, left),
        copy(11, lab_ref, lab_diag, up_left),
    ]
    for c in first + weights[0] + label_copies + second + weights[1]:
        c.start()

    lane = lax.broadcasted_iota(jnp.int32, (1, C), 1)
    head_of = lane // HEAD
    heads = [(head_of == h).astype(F32).astype(BF) for h in range(HEADS)]

    for b in range(2):
        wproj[b, 0:64] = projw_ref[b]

    for c in first:
        c.wait_recv()

    def merge(b):
        wqkv[b, :, 0:128] = side_by_side(qkvw_ref[b, 0], qk_r[b, :, 0:64]).astype(BF)
        wqkv[b, :, 128:256] = side_by_side(qkvw_ref[b, 1], qk_r[b, :, 64:128]).astype(BF)
        wqkv[b, :, 256:384] = side_by_side(
            qkvw_ref[b, 2], v_r[:, 64 * b : 64 * b + 64]
        ).astype(BF)
        bqkv[b, 0:3] = side_by_side(qkvb_ref[b], qkvb_r[b])

    rel = rel_ref[...]
    low = rel < 128
    within = jnp.bitwise_and(rel, 127)
    left_half = lane < 64
    for b in range(2):
        for tile, source in enumerate((tbl_ref, tbl_r)):
            picked = []
            for h in range(2):
                row = 4 * b + 2 * h
                a0 = jnp.broadcast_to(source[row : row + 1], rel.shape)
                a1 = jnp.broadcast_to(source[row + 1 : row + 2], rel.shape)
                g0 = jnp.take_along_axis(a0, within, axis=1)
                g1 = jnp.take_along_axis(a1, within, axis=1)
                picked.append(jnp.where(low, g0, g1))
            bias[b, :, 128 * tile : 128 * tile + 128] = (
                jnp.where(left_half, picked[0], picked[1]) * LOG2E
            )

    def qkv(b, tokens):
        n = norm(tokens, gain_ref[b, 0:1], shift_ref[b, 0:1])
        r = dot(n, wqkv[b])
        q = ((r[:, 0:128] + bqkv[b, 0:1]) * QSCALE).astype(BF)
        k = (r[:, 128:256] + bqkv[b, 1:2]).astype(BF)
        v = (r[:, 256:384] + bqkv[b, 2:3]).astype(BF)
        return q, k, v

    def attend(b, q, k, v, allowed):
        stacked = jnp.concatenate([q * m for m in heads], axis=0)
        s = lax.dot_general(
            k, stacked, (((1,), (1,)), ((), ())), preferred_element_type=F32
        )
        s = s + bias[b]
        if allowed is not None:
            s = jnp.concatenate(
                [jnp.where(allowed, s[:, 0:128], EXCLUDED),
                 jnp.where(allowed, s[:, 128:256], EXCLUDED)], axis=1)
        raised = jnp.exp2(s - jnp.max(s, axis=0, keepdims=True))
        w = (raised * (1.0 / jnp.sum(raised, axis=0, keepdims=True))).astype(BF)
        o = lax.dot_general(w, v, (((0,), (0,)), ((), ())), preferred_element_type=F32)
        mixed = o[192:256]
        for h in (2, 1, 0):
            mixed = jnp.where(head_of == h, o[64 * h : 64 * h + 64], mixed)
        return mixed.astype(BF)

    def feed(b, attended, tokens, proj):
        mid = (tokens + dot(attended, proj) + projb_ref[b : b + 1]).astype(BF).astype(F32)
        n = norm(mid, gain_ref[b, 1:2], shift_ref[b, 1:2])
        total = mid + fc2b_ref[b : b + 1]
        for w1, b1, w2 in (
            (fc1w_ref, fc1b_ref, fc2w_ref), (fc1w_r, fc1b_r, fc2w_r)
        ):
            inner = dot(n, w1[b]) + b1[b : b + 1]
            hidden = (inner * (0.5 + 0.5 * lax.erf(inner * ROOT_HALF))).astype(BF)
            total = total + dot(hidden, w2[b])
        return total.astype(BF).astype(F32)

    def slab(r, at):
        return y[r, pl.ds(at, WIN), :]

    merge(0)
    for c in weights[0]:
        c.wait_recv()

    def halo_copy(j):
        at = pl.ds(pl.multiple_of(j * CHUNK, CHUNK), CHUNK)
        return copy(20 + j, halo_s.at[:, at], halo_r.at[:, at], up)

    def first_block(j, carry):
        base = pl.multiple_of(j * CHUNK, CHUNK)
        rows = [x_ref[r, pl.ds(base, CHUNK), :].astype(F32) for r in range(WIN)]
        tokens = jnp.concatenate(
            [rows[r][WIN * g : WIN * g + WIN] for g in range(GROUP) for r in range(WIN)], axis=0
        )
        q, k, v = qkv(0, tokens)
        attended = jnp.concatenate(
            [attend(0, *(a[64 * g : 64 * g + 64] for a in (q, k, v)), None) for g in range(GROUP)],
            axis=0,
        )
        done = feed(0, attended, tokens, wproj[0])
        for r in range(WIN):
            line = jnp.concatenate(
                [done[64 * g + 8 * r : 64 * g + 8 * r + 8] for g in range(GROUP)], axis=0
            )
            y[r, pl.ds(base, CHUNK), :] = line
            if r < SHIFT:
                halo_s[r, pl.ds(base, CHUNK), :] = line.astype(BF)
        halo_copy(j).start()
        return carry

    lax.fori_loop(0, chunks, first_block, 0)

    for r in range(SHIFT):
        side_s[r] = y[SHIFT + r, 0:16, :].astype(BF)
    patches = [
        copy(12 + 28, side_s, side_r, left),
        copy(13 + 28, halo_s.at[:, pl.ds(0, 16)], diag_r, up_left),
    ]
    for c in patches:
        c.start()

    for c in label_copies:
        c.wait_recv()
    last_band = (band == bands - 1).astype(jnp.int32) * 2
    last_tile = (col == tiles - 1).astype(jnp.int32)
    for r in range(WIN):
        if r < SHIFT:
            own, beside, extra = lab_ref, lab_side, 0
            at = SHIFT + r
        else:
            own, beside, extra = lab_up, lab_diag, last_band
            at = r - SHIFT
        for t in range(cols // 128):
            line = own[at : at + 1, 128 * t : 128 * t + 128] * 4 + extra
            ids[r, 128 * t : 128 * t + 128, :] = jnp.broadcast_to(line.astype(F32), (128, 128)).T
        line = beside[at : at + 1, 0:128] * 4 + extra + last_tile
        ids[r, cols : cols + 8, :] = jnp.broadcast_to(line.astype(F32), (128, 128)).T[0:8]

    for c in second:
        c.wait_recv()
    merge(1)

    for j in range(chunks):
        halo_copy(j).wait_recv()
    for c in patches:
        c.wait_recv()
    for r in range(SHIFT):
        y[WIN + r, 0:cols, :] = halo_r[r].astype(F32)
        y[SHIFT + r, cols : cols + 8, :] = side_r[r].astype(F32)[0:8]
        y[WIN + r, cols : cols + 8, :] = diag_r[r].astype(F32)[0:8]

    def attended_copy(j):
        at = pl.ds(pl.multiple_of(j * 32 * GROUP, 32 * GROUP), 32 * GROUP)
        return copy(28 + j, att_s.at[at], att_r.at[at], down)

    def second_attention(j, carry):
        base = pl.multiple_of(j * CHUNK, CHUNK)
        tokens = jnp.concatenate(
            [slab(SHIFT + r, base + SHIFT + WIN * g) for g in range(GROUP) for r in range(WIN)],
            axis=0,
        )
        q, k, v = qkv(1, tokens)
        for g in range(GROUP):
            mine = jnp.concatenate(
                [ids[r, pl.ds(base + SHIFT + WIN * g, WIN), :] for r in range(WIN)], axis=0
            )
            other = jnp.concatenate([mine, mine], axis=0).T[0:64]
            o = attend(1, *(a[64 * g : 64 * g + 64] for a in (q, k, v)), mine == other)
            at = pl.ds(pl.multiple_of(j * 32 * GROUP, 32 * GROUP) + 32 * g, 32)
            att_own[at, :] = o[0:32]
            att_s[at, :] = o[32:64]
        attended_copy(j).start()
        return carry

    lax.fori_loop(0, chunks, second_attention, 0)

    final = pl.ds(32 * (wins - 1), 32)
    corner_copies = [
        copy(42, att_own.at[final], att_side, right),
        copy(43, att_s.at[final], att_diag, down_right),
    ]
    for c in corner_copies:
        c.start()
    for r in range(WIN):
        y[r, cols : cols + 8, :] = y[r, 0:8, :]
    for c in weights[1]:
        c.wait_recv()
    wturned[0:64] = wproj[1, 64:128]
    wturned[64:128] = wproj[1, 0:64]

    def second_feed(attended_ref, first_row, proj):
        def body(j, carry):
            base = pl.multiple_of(j * CHUNK, CHUNK)
            at = pl.ds(pl.multiple_of(j * 32 * GROUP, 32 * GROUP), 32 * GROUP)
            where = [
                (first_row + r, base + SHIFT + WIN * g) for g in range(GROUP) for r in range(SHIFT)
            ]
            tokens = jnp.concatenate([slab(*w) for w in where], axis=0)
            done = feed(1, attended_ref[at, :], tokens, proj[...])
            for i, (r, c) in enumerate(where):
                y[r, pl.ds(c, WIN), :] = done[8 * i : 8 * i + 8]
            return carry

        lax.fori_loop(0, chunks, body, 0)

    right_part = jnp.bitwise_and(lax.broadcasted_iota(jnp.int32, (32, C), 0), 7) >= SHIFT
    def put_corner(target, source):
        target[final, :] = jnp.where(
            right_part, source[...].astype(F32), target[final, :].astype(F32)
        ).astype(BF)

    corner_copies[0].wait()
    put_corner(att_own, att_side)
    second_feed(att_own, SHIFT, wproj.at[1])
    for j in range(chunks):
        attended_copy(j).wait_recv()
    corner_copies[1].wait()
    put_corner(att_r, att_diag)
    second_feed(att_r, 0, wturned)

    for r in range(WIN):
        head_cols = y[r, cols : cols + 8, :]
        keep = lax.broadcasted_iota(jnp.int32, (8, C), 0) < SHIFT
        y[r, 0:8, :] = jnp.where(keep, head_cols, y[r, 0:8, :])
        out_ref[r] = y[r, 0:cols, :].astype(BF)

    for c in first + second + weights[0] + weights[1] + label_copies + patches:
        c.wait_send()
    for j in range(chunks):
        halo_copy(j).wait_send()
        attended_copy(j).wait_send()


def on_device(
    image_tokens, labels, rel_index, norm_gain, norm_shift, qkv_weight, qkv_bias, bias_table,
    proj_weight, proj_bias, fc1_weight, fc1_bias, fc2_weight, fc2_bias,
):
    rows, cols, _ = image_tokens.shape
    wins = cols // WIN
    rel = jnp.tile(rel_index.T, (1, 2))
    entries = bias_table.shape[1]
    table = jnp.pad(
        jnp.transpose(bias_table, (0, 2, 1)), ((0, 0), (0, 0), (0, 256 - entries))
    ).reshape(8, 128)
    vmem = pl.BlockSpec(memory_space=pltpu.VMEM)
    args = (
        image_tokens, labels, rel, norm_gain, norm_shift, qkv_weight, qkv_bias, table,
        proj_weight, proj_bias, fc1_weight, fc1_bias, fc2_weight, fc2_bias,
    )
    V = pltpu.VMEM
    copies = 44
    return pl.pallas_call(
        kernel,
        out_shape=jax.ShapeDtypeStruct((rows, cols, C), BF),
        in_specs=[vmem] * len(args),
        out_specs=vmem,
        scratch_shapes=[
            V((rows + SHIFT, cols + 8, C), F32),
            V((rows, cols + 8, C), F32),
            V((2, C, 3 * C), BF),
            V((2, 3, C), F32),
            V((2, C, C), BF),
            V((C, C), BF),
            V((2, 64, 256), F32),
            V((2, C, C), BF), V((2, C, C), BF),
            V((C, C), BF), V((C, C), BF),
            V(qkv_bias.shape, F32), V((8, 128), F32), V(fc1_bias.shape, F32),
            V(fc1_weight.shape, BF), V(fc2_weight.shape, BF),
            V(labels.shape, jnp.int32), V(labels.shape, jnp.int32), V(labels.shape, jnp.int32),
            V((SHIFT, cols, C), BF), V((SHIFT, cols, C), BF),
            V((SHIFT, 16, C), BF), V((SHIFT, 16, C), BF), V((SHIFT, 16, C), BF),
            V((32 * wins, C), BF), V((32 * wins, C), BF), V((32 * wins, C), BF),
            V((32, C), BF), V((32, C), BF),
            pltpu.SemaphoreType.DMA((copies,)),
            pltpu.SemaphoreType.DMA((copies,)),
        ],
        compiler_params=pltpu.CompilerParams(
            collective_id=0, has_side_effects=True, vmem_limit_bytes=60 * 1024 * 1024
        ),
        name="swin_pair",
    )(*args)


def solution(mesh):
    in_specs = (
        P(("row", "ch"), "col", None),
        P(("row", "ch"), "col"),
        P(),
        P(),
        P(),
        P(None, None, None, "ch"),
        P(None, None, "ch"),
        P(None, None, "ch"),
        P(None, "ch", None),
        P(),
        P(None, None, "ch"),
        P(None, "ch"),
        P(None, "ch", None),
        P(),
    )
    out_specs = P(("row", "ch"), "col", None)
    return jax.shard_map(
        on_device, mesh=mesh, in_specs=in_specs, out_specs=out_specs, check_vma=False
    )
```

```python
import functools
import math

import jax
import jax.numpy as jnp
from jax import lax
from jax.experimental import pallas as pl
from jax.experimental.pallas import tpu as pltpu
from jax.sharding import PartitionSpec as P

WIN = 8
SHIFT = 4
HEADS = 4
EPS = 1e-05
C = 128
HEAD = 32
BF = jnp.bfloat16
F32 = jnp.float32
LOG2E = math.log2(math.e)
QSCALE = LOG2E / math.sqrt(HEAD)
ROOT_HALF = math.sqrt(0.5)
EXCLUDED = -1e30
MESH = pl.DeviceIdType.MESH

GROUP = 8
CHUNK = GROUP * WIN
SPANS = 3


def norm(x, gain, shift):
    center = x - jnp.mean(x, axis=-1, keepdims=True)
    spread = jnp.mean(center * center, axis=-1, keepdims=True)
    return (center * lax.rsqrt(spread + EPS) * gain + shift).astype(BF)


def dot(a, b):
    return jnp.dot(a, b, preferred_element_type=F32)


def dot_rows(a, b):
    return lax.dot_general(a, b, (((1,), (1,)), ((), ())), preferred_element_type=F32)


def dot_first(a, b):
    return lax.dot_general(a, b, (((0,), (0,)), ((), ())), preferred_element_type=F32)


def kernel(
    x_in, lab_in, rel_in, gain_in, shift_in, qkvw_in, qkvb_in, tbl_in, projw_in,
    projb_in, fc1w_in, fc1b_in, fc2w_in, fc2b_in,
    out_ref,
    x, lab, rel, gain, shift, qkvb, tbl, wproj, projb, w1, b1, w2, fc2b,
    wown, woth, wfull, bqkv, bias0, bias1,
    y, ids, normed, att, result, region, labs,
    halo, both, sides, corners,
    local, send, recv,
):
    cols = x.shape[1]
    chunks = cols // CHUNK
    wins = cols // WIN + 1
    span = wins // SPANS
    groups = lax.axis_size("ch")
    bands = lax.axis_size("row") * groups
    tiles = lax.axis_size("col")
    ch = lax.axis_index("ch")
    col = lax.axis_index("col")
    band = lax.axis_index("row") * groups + ch

    def device(band_step, col_step):
        b = lax.rem(band + bands + band_step, bands)
        c = lax.rem(col + tiles + col_step, tiles)
        return {"row": b // groups, "col": c, "ch": lax.rem(b, groups)}

    partner = {"row": lax.axis_index("row"), "col": col, "ch": 1 - ch}
    up, down = device(-1, 0), device(1, 0)
    left, right = device(0, -1), device(0, 1)
    diagonals = [device(i, j) for i in (-1, 1) for j in (-1, 1)]

    barrier = pltpu.get_barrier_semaphore()
    peers = [up, down, left, right] + diagonals
    for peer in peers:
        pl.semaphore_signal(barrier, inc=1, device_id=peer, device_id_type=MESH)

    def load(i, src, dst):
        return pltpu.make_async_copy(src, dst, local.at[i])

    own_rows = pl.ds(0, 64)
    other_rows = pl.ds(64, 64)
    early = [
        load(0, x_in, x),
        load(1, qkvw_in.at[0], wown.at[:, own_rows]),
        load(2, qkvb_in, qkvb.at[0]),
        load(3, tbl_in, tbl.at[0]),
        load(4, rel_in, rel),
        load(5, gain_in, gain),
        load(6, shift_in, shift),
    ]
    late = [
        load(7, projw_in, wproj.at[:, own_rows]),
        load(8, fc1w_in, w1.at[0]),
        load(9, fc1b_in, b1.at[0]),
        load(10, fc2w_in, w2.at[0]),
        load(11, qkvw_in.at[1], wfull.at[:, own_rows]),
        load(12, projb_in, projb),
        load(13, fc2b_in, fc2b),
        load(14, lab_in, lab),
    ]
    for c in early + late:
        c.start()

    wown[:, 64:128, :] = jnp.zeros((3, 64, C), BF)
    woth[:, 0:64, :] = jnp.zeros((3, 64, C), BF)

    def copy(i, src, dst, to):
        return pltpu.make_async_remote_copy(
            src_ref=src, dst_ref=dst, send_sem=send.at[i], recv_sem=recv.at[i],
            device_id=to, device_id_type=MESH,
        )

    first = [
        copy(0, wown.at[:, own_rows], woth.at[:, other_rows], partner),
        copy(1, qkvb.at[0], qkvb.at[1], partner),
        copy(2, tbl.at[0], tbl.at[1], partner),
        copy(3, b1.at[0], b1.at[1], partner),
    ]
    def feed_copies(b):
        return [
            copy(4 + 4 * b, wproj.at[b, own_rows], wproj.at[b, other_rows], partner),
            copy(5 + 4 * b, w1.at[0, b], w1.at[1, b], partner),
            copy(6 + 4 * b, w2.at[0, b], w2.at[1, b], partner),
        ]
    second = feed_copies(0)
    third = [copy(7, wfull.at[:, own_rows], wfull.at[:, other_rows], partner)] + feed_copies(1)
    half_at = {-1: pl.ds(0, 128), 1: pl.ds(cols - 128, 128)}
    region_copies = [copy(11, region, labs.at[0], up), copy(12, region, labs.at[1], down)] + [
        copy(13 + i, region.at[:, half_at[side]], labs.at[2 + i, :, pl.ds(0, 128)], to)
        for i, (side, to) in enumerate(
            [(-1, left), (1, right)] + list(zip((-1, 1, -1, 1), diagonals))
        )
    ]

    for c in early:
        c.wait()

    lane = lax.broadcasted_iota(jnp.int32, (1, C), 1)
    head_of = lane // HEAD
    heads = [(head_of == h).astype(F32).astype(BF) for h in range(HEADS)]

    entries = tbl.shape[-1]
    relt = rel[...].astype(F32).T

    def lookup(index, side, b, h):
        index = index.astype(jnp.int32)
        line = tbl[side, b, h : h + 1, :]
        a0 = jnp.broadcast_to(line[:, 0:128], index.shape)
        a1 = jnp.concatenate([line[:, 128:], jnp.zeros((1, 256 - entries), F32)], axis=1)
        a1 = jnp.broadcast_to(a1, index.shape)
        within = jnp.bitwise_and(index, 127)
        g0 = jnp.take_along_axis(a0, within, axis=1)
        g1 = jnp.take_along_axis(a1, within, axis=1)
        return jnp.where(index < 128, g0, g1) * LOG2E

    twice = jnp.concatenate([relt, relt], axis=1)

    def first_bias(side):
        bias0[:, 128 * side : 128 * side + 128] = jnp.where(
            lane < 64, lookup(twice, side, 0, 0), lookup(twice, side, 0, 1)
        )

    def zero_padded(values, side):
        pad = jnp.zeros_like(values)
        return jnp.concatenate([values, pad] if side == 0 else [pad, values], axis=1)

    first_bias(0)
    for m in range(3):
        bqkv[0, m : m + 1] = zero_padded(qkvb[0, m, 0:1], 0)

    def project(n, w, b):
        r = dot_rows(n, w[...].reshape(3 * C, C))
        q = ((r[:, 0:128] + bqkv[b, 0:1]) * QSCALE).astype(BF)
        k = (r[:, 128:256] + bqkv[b, 1:2]).astype(BF)
        v = (r[:, 256:384] + bqkv[b, 2:3]).astype(BF)
        return q, k, v

    def softmax(s):
        raised = jnp.exp2(s - jnp.max(s, axis=0, keepdims=True))
        return (raised * (1.0 / jnp.sum(raised, axis=0, keepdims=True))).astype(BF)

    def half_attention(side, q, k, v):
        stacked = jnp.concatenate([q * heads[2 * side], q * heads[2 * side + 1]], axis=0)
        s = dot_rows(k, stacked) + bias0[:, 128 * side : 128 * side + 128]
        o = dot_first(softmax(s), v)
        return jnp.where(head_of == 2 * side, o[0:64], o[64:128]).astype(BF)

    def windows_of(base):
        lines = [x[r, pl.ds(base, CHUNK), :].astype(F32) for r in range(WIN)]
        return jnp.concatenate(
            [lines[r][WIN * g : WIN * g + WIN] for g in range(GROUP) for r in range(WIN)], axis=0
        )

    def own_heads(j, carry):
        base = pl.multiple_of(j * CHUNK, CHUNK)
        at = pl.ds(pl.multiple_of(j * 64 * GROUP, 64 * GROUP), 64 * GROUP)
        n = norm(windows_of(base), gain[0, 0:1], shift[0, 0:1])
        normed[at, :] = n
        q, k, v = project(n, wown, 0)
        att[at, :] = jnp.concatenate(
            [half_attention(0, *(a[64 * g : 64 * g + 64] for a in (q, k, v))) for g in range(GROUP)],
            axis=0,
        )
        return carry

    lax.fori_loop(0, chunks, own_heads, 0)

    for c in late:
        c.wait()
    i = lax.broadcasted_iota(jnp.int32, lab.shape, 0)
    j = lax.broadcasted_iota(jnp.int32, lab.shape, 1)
    first_band = (band == 0).astype(jnp.int32)
    first_tile = (col == 0).astype(jnp.int32)
    region[...] = (
        lab[...] * 4
        + (i < SHIFT).astype(jnp.int32) * (2 * first_band)
        + (j < SHIFT).astype(jnp.int32) * first_tile
    )

    pl.semaphore_wait(barrier, len(peers))
    for c in first + second + region_copies + third:
        c.start()

    for c in first:
        c.wait_recv()
    first_bias(1)
    for m in range(3):
        bqkv[1, m : m + 1] = zero_padded(qkvb[1, m, 0:1], 1)
        bqkv[2, m : m + 1] = jnp.concatenate([qkvb[0, m, 1:2], qkvb[1, m, 1:2]], axis=1)
    for t, turned in enumerate(
        (relt[:, 0:32], jnp.concatenate([relt[32:64, 32:64], relt[0:32, 32:64]], axis=0))
    ):
        index = jnp.concatenate([turned] * 4, axis=1)
        picked = lookup(index, 1, 1, 1)
        for h in (2, 1, 0):
            picked = jnp.where(head_of == h, lookup(index, h // 2, 1, h % 2), picked)
        bias1[t] = picked

    def feed(b, attended, tokens):
        mid = (tokens + dot(attended, wproj[b]) + projb[b : b + 1]).astype(BF).astype(F32)
        n = norm(mid, gain[b, 1:2], shift[b, 1:2])
        total = mid + fc2b[b : b + 1]
        for side in range(2):
            inner = dot(n, w1[side, b]) + b1[side, b : b + 1]
            hidden = (inner * (0.5 + 0.5 * lax.erf(inner * ROOT_HALF))).astype(BF)
            total = total + dot(hidden, w2[side, b])
        return total.astype(BF).astype(F32)

    for c in second:
        c.wait_recv()

    def halo_copies(k):
        at = pl.ds(pl.multiple_of(k * CHUNK, CHUNK), CHUNK)
        return (
            copy(20 + k, halo.at[pl.ds(0, SHIFT), at], both.at[0, :, at], up),
            copy(24 + k, halo.at[pl.ds(SHIFT, SHIFT), at], both.at[1, :, at], down),
        )

    def first_block(k, carry):
        base = pl.multiple_of(k * CHUNK, CHUNK)
        at = pl.ds(pl.multiple_of(k * 64 * GROUP, 64 * GROUP), 64 * GROUP)
        q, key, v = project(normed[at, :], woth, 1)
        other = jnp.concatenate(
            [half_attention(1, *(a[64 * g : 64 * g + 64] for a in (q, key, v))) for g in range(GROUP)],
            axis=0,
        )
        done = feed(0, att[at, :] + other, windows_of(base))
        for r in range(WIN):
            line = jnp.concatenate(
                [done[64 * g + 8 * r : 64 * g + 8 * r + 8] for g in range(GROUP)], axis=0
            )
            y[SHIFT + r, pl.ds(base + SHIFT, CHUNK), :] = line
            halo[r, pl.ds(base, CHUNK), :] = line.astype(BF)
        for c in halo_copies(k):
            c.start()
        return carry

    lax.fori_loop(0, chunks, first_block, 0)

    edge = {-1: pl.ds(0, 16), 1: pl.ds(cols - 16, 16)}
    edge_copies = [
        copy(28, halo.at[:, edge[-1]], sides.at[1], left),
        copy(29, halo.at[:, edge[1]], sides.at[0], right),
    ] + [
        copy(30 + i, halo.at[pl.ds(r0, SHIFT), edge[side]], corners.at[i], to)
        for i, ((r0, side), to) in enumerate(
            zip(((0, -1), (0, 1), (SHIFT, -1), (SHIFT, 1)), diagonals)
        )
    ]
    for c in edge_copies:
        c.start()

    for c in region_copies:
        c.wait_recv()

    def spread(line):
        return jnp.broadcast_to(line.astype(F32), (128, 128)).T

    for r in range(2 * WIN):
        if r < SHIFT:
            middle, before, after, at = labs.at[1], labs.at[7], labs.at[6], SHIFT + r
        elif r < SHIFT + WIN:
            middle, before, after, at = region, labs.at[3], labs.at[2], r - SHIFT
        else:
            middle, before, after, at = labs.at[0], labs.at[5], labs.at[4], r - SHIFT - WIN
        for t in range(cols // 128):
            ids[r, SHIFT + 128 * t : SHIFT + 128 * t + 128, :] = spread(
                middle[at : at + 1, 128 * t : 128 * t + 128]
            )
        ids[r, 0:SHIFT, :] = spread(before[at : at + 1, 0:128])[128 - SHIFT :]
        ids[r, SHIFT + cols : 2 * SHIFT + cols, :] = spread(after[at : at + 1, 0:128])[0:SHIFT]

    for c in third:
        c.wait_recv()
    for c in edge_copies[0:2]:
        c.wait_recv()
    ends = ((slice(0, SHIFT), slice(12, 16)), (slice(SHIFT + cols, 2 * SHIFT + cols), slice(0, SHIFT)))
    for s, (to, of) in enumerate(ends):
        for r in range(WIN):
            y[SHIFT + r, to, :] = sides[s, r].astype(F32)[of]

    def shifted_band(is_bottom):
        mine = SHIFT + SHIFT * is_bottom
        theirs = (SHIFT + WIN) * is_bottom

        arrived = both.at[1 - is_bottom]
        flow = 20 + 4 * (1 - is_bottom)

        def take(k):
            at = pl.ds(pl.multiple_of(k * CHUNK, CHUNK), CHUNK)
            copy(flow + k, arrived.at[:, at], arrived.at[:, at], up).wait_recv()
            for r in range(SHIFT):
                y[theirs + r, pl.ds(k * CHUNK + SHIFT, CHUNK), :] = arrived[r, at, :].astype(F32)

        corner = 2 * (1 - is_bottom)
        for i in range(2):
            part = corners.at[corner + i]
            copy(30 + corner + i, part, part, up).wait_recv()
            to, of = ends[1 - i]
            for r in range(SHIFT):
                y[theirs + r, to, :] = part[r].astype(F32)[of]
        take(0)

        def body(c, carry):
            take(c + 1)
            base = pl.multiple_of(c * span * WIN, WIN)

            def gather(ref, row):
                return [
                    [ref[row + r, pl.ds(base + WIN * g, WIN), :] for r in range(SHIFT)]
                    for g in range(span)
                ]

            own = gather(y, mine)
            beside = gather(y, theirs)
            own_id = gather(ids, mine)
            beside_id = gather(ids, theirs)
            flat = lambda parts: jnp.concatenate([p for g in parts for p in g], axis=0)
            tokens = flat(own)
            n = norm(tokens, gain[1, 0:1], shift[1, 0:1])
            n2 = norm(flat(beside), gain[1, 0:1], shift[1, 0:1])
            q, k, v = project(n, wfull, 2)
            r2 = dot_rows(n2, wfull[1:3].reshape(2 * C, C))
            k2 = (r2[:, 0:128] + bqkv[2, 1:2]).astype(BF)
            v2 = (r2[:, 128:256] + bqkv[2, 2:3]).astype(BF)
            attended = []
            for g in range(span):
                at = slice(32 * g, 32 * g + 32)
                keys = jnp.concatenate([k[at], k2[at]], axis=0)
                values = jnp.concatenate([v[at], v2[at]], axis=0)
                stacked = jnp.concatenate([q[at] * m for m in heads], axis=0)
                s = dot_rows(keys, stacked) + bias1[1 - is_bottom]
                key_id = jnp.concatenate(own_id[g] + beside_id[g], axis=0)
                query_id = jnp.concatenate(own_id[g] * 4, axis=0).T[0:8]
                allowed = key_id == jnp.concatenate([query_id] * 8, axis=0)
                o = dot_first(softmax(jnp.where(allowed, s, EXCLUDED)), values)
                mixed = o[96:128]
                for h in (2, 1, 0):
                    mixed = jnp.where(head_of == h, o[32 * h : 32 * h + 32], mixed)
                attended.append(mixed.astype(BF))
            done = feed(1, jnp.concatenate(attended, axis=0), tokens)
            for g in range(span):
                for r in range(SHIFT):
                    i = 32 * g + 8 * r
                    y[mine + r, pl.ds(base + WIN * g, WIN), :] = done[i : i + 8]
            return carry

        lax.fori_loop(0, SPANS, body, 0)
        row = SHIFT * is_bottom
        for r in range(SHIFT):
            result[row + r] = y[mine + r, SHIFT : SHIFT + cols, :].astype(BF)
        return pltpu.make_async_copy(
            result.at[pl.ds(row, SHIFT)], out_ref.at[pl.ds(row, SHIFT)], local.at[15 + is_bottom]
        )

    near = 1 - ch
    outs = []
    for is_bottom in (near, 1 - near):
        c = shifted_band(is_bottom)
        c.start()
        outs.append(c)
    for c in outs:
        c.wait()

    for c in first + second + third + region_copies + edge_copies:
        c.wait_send()
    for k in range(chunks):
        for c in halo_copies(k):
            c.wait_send()


def on_device(
    image_tokens, labels, rel_index, norm_gain, norm_shift, qkv_weight, qkv_bias, bias_table,
    proj_weight, proj_bias, fc1_weight, fc1_bias, fc2_weight, fc2_bias,
):
    rows, cols, _ = image_tokens.shape
    args = (
        image_tokens, labels, rel_index, norm_gain, norm_shift,
        jnp.swapaxes(qkv_weight, 2, 3), jnp.swapaxes(qkv_bias, 0, 1),
        jnp.swapaxes(bias_table, 1, 2),
        proj_weight, proj_bias, fc1_weight, fc1_bias, fc2_weight, fc2_bias,
    )
    V = pltpu.VMEM
    like = lambda a, *lead: V((*lead, *a.shape), a.dtype)
    copies = 34
    return pl.pallas_call(
        kernel,
        out_shape=jax.ShapeDtypeStruct((rows, cols, C), BF),
        in_specs=[pl.BlockSpec(memory_space=pl.ANY)] * len(args),
        out_specs=pl.BlockSpec(memory_space=pl.ANY),
        scratch_shapes=[
            like(image_tokens), like(labels), like(rel_index), like(norm_gain), like(norm_shift),
            like(args[6], 2), like(args[7], 2),
            V((2, C, C), BF), like(proj_bias),
            like(fc1_weight, 2), like(fc1_bias, 2), like(fc2_weight, 2), like(fc2_bias),
            V((3, C, C), BF), V((3, C, C), BF), V((3, C, C), BF),
            V((3, 3, C), F32),
            V((64, 256), F32), V((2, 64, C), F32),
            V((2 * WIN, cols + 8, C), F32), V((2 * WIN, cols + 8, C), F32),
            V((rows * cols, C), BF), V((rows * cols, C), BF),
            V((rows, cols, C), BF),
            like(labels), like(labels, 8),
            V((rows, cols, C), BF), V((2, SHIFT, cols, C), BF),
            V((2, rows, 16, C), BF), V((4, SHIFT, 16, C), BF),
            pltpu.SemaphoreType.DMA((17,)),
            pltpu.SemaphoreType.DMA((copies,)),
            pltpu.SemaphoreType.DMA((copies,)),
        ],
        compiler_params=pltpu.CompilerParams(
            collective_id=0, has_side_effects=True, vmem_limit_bytes=60 * 1024 * 1024
        ),
        name="swin_pair",
    )(*args)


def solution(mesh):
    in_specs = (
        P(("row", "ch"), "col", None),
        P(("row", "ch"), "col"),
        P(),
        P(),
        P(),
        P(None, None, None, "ch"),
        P(None, None, "ch"),
        P(None, None, "ch"),
        P(None, "ch", None),
        P(),
        P(None, None, "ch"),
        P(None, "ch"),
        P(None, "ch", None),
        P(),
    )
    out_specs = P(("row", "ch"), "col", None)
    return jax.shard_map(
        on_device, mesh=mesh, in_specs=in_specs, out_specs=out_specs, check_vma=False
    )
```

```python
import functools
import math

import jax
import jax.numpy as jnp
from jax import lax
from jax.experimental import pallas as pl
from jax.experimental.pallas import tpu as pltpu
from jax.sharding import PartitionSpec as P

WIN = 8
SHIFT = 4
HEADS = 4
EPS = 1e-05
C = 128
HEAD = 32
BF = jnp.bfloat16
F32 = jnp.float32
LOG2E = math.log2(math.e)
QSCALE = LOG2E / math.sqrt(HEAD)
ROOT_HALF = math.sqrt(0.5)
EXCLUDED = -1e30
MESH = pl.DeviceIdType.MESH

GROUP = 8
CHUNK = GROUP * WIN
SPANS = 3


def norm(x, gain, shift):
    center = x - jnp.mean(x, axis=-1, keepdims=True)
    spread = jnp.mean(center * center, axis=-1, keepdims=True)
    return (center * lax.rsqrt(spread + EPS) * gain + shift).astype(BF)


def dot(a, b):
    return jnp.dot(a, b, preferred_element_type=F32)


def dot_rows(a, b):
    return lax.dot_general(a, b, (((1,), (1,)), ((), ())), preferred_element_type=F32)


def kernel(
    x_in, lab_in, rel_in, gain_in, shift_in, qkvw_in, qkvb_in, tbl_in, projw_in,
    projb_in, fc1w_in, fc1b_in, fc2w_in, fc2b_in,
    out_ref,
    x, lab, rel, gain, shift, qkvb, tbl, wproj, projb, w1, b1, w2, fc2b,
    wown, woth, wfull, bqkv, bias0, bias1,
    y, ids, normed, att, result, region, labs,
    halo, both, sides, corners,
    local, send, recv,
):
    cols = x.shape[1]
    chunks = cols // CHUNK
    wins = cols // WIN + 1
    span = wins // SPANS
    groups = lax.axis_size("ch")
    bands = lax.axis_size("row") * groups
    tiles = lax.axis_size("col")
    ch = lax.axis_index("ch")
    col = lax.axis_index("col")
    band = lax.axis_index("row") * groups + ch

    def device(band_step, col_step):
        b = lax.rem(band + bands + band_step, bands)
        c = lax.rem(col + tiles + col_step, tiles)
        return {"row": b // groups, "col": c, "ch": lax.rem(b, groups)}

    partner = {"row": lax.axis_index("row"), "col": col, "ch": 1 - ch}
    up, down = device(-1, 0), device(1, 0)
    left, right = device(0, -1), device(0, 1)
    diagonals = [device(i, j) for i in (-1, 1) for j in (-1, 1)]

    barrier = pltpu.get_barrier_semaphore()
    peers = [up, down, left, right] + diagonals
    for peer in peers:
        pl.semaphore_signal(barrier, inc=1, device_id=peer, device_id_type=MESH)

    def load(i, src, dst):
        return pltpu.make_async_copy(src, dst, local.at[i])

    own_rows = pl.ds(0, 64)
    other_rows = pl.ds(64, 64)
    early = [
        load(0, x_in, x),
        load(1, qkvw_in.at[0], wown.at[:, own_rows]),
        load(2, qkvb_in, qkvb.at[0]),
        load(3, tbl_in, tbl.at[0]),
        load(4, rel_in, rel),
        load(5, gain_in, gain),
        load(6, shift_in, shift),
    ]
    late = [
        load(7, projw_in, wproj.at[:, own_rows]),
        load(8, fc1w_in, w1.at[0]),
        load(9, fc1b_in, b1.at[0]),
        load(10, fc2w_in, w2.at[0]),
        load(11, qkvw_in.at[1], wfull.at[:, own_rows]),
        load(12, projb_in, projb),
        load(13, fc2b_in, fc2b),
        load(14, lab_in, lab),
    ]
    for c in early + late:
        c.start()

    wown[:, 64:128, :] = jnp.zeros((3, 64, C), BF)
    woth[:, 0:64, :] = jnp.zeros((3, 64, C), BF)

    def copy(i, src, dst, to):
        return pltpu.make_async_remote_copy(
            src_ref=src, dst_ref=dst, send_sem=send.at[i], recv_sem=recv.at[i],
            device_id=to, device_id_type=MESH,
        )

    first = [
        copy(0, wown.at[:, own_rows], woth.at[:, other_rows], partner),
        copy(1, qkvb.at[0], qkvb.at[1], partner),
        copy(2, tbl.at[0], tbl.at[1], partner),
        copy(3, b1.at[0], b1.at[1], partner),
    ]
    def feed_copies(b):
        return [
            copy(4 + 4 * b, wproj.at[b, own_rows], wproj.at[b, other_rows], partner),
            copy(5 + 4 * b, w1.at[0, b], w1.at[1, b], partner),
            copy(6 + 4 * b, w2.at[0, b], w2.at[1, b], partner),
        ]
    second = feed_copies(0)
    third = [copy(7, wfull.at[:, own_rows], wfull.at[:, other_rows], partner)] + feed_copies(1)
    half_at = {-1: pl.ds(0, 128), 1: pl.ds(cols - 128, 128)}
    region_copies = [copy(11, region, labs.at[0], up), copy(12, region, labs.at[1], down)] + [
        copy(13 + i, region.at[:, half_at[side]], labs.at[2 + i, :, pl.ds(0, 128)], to)
        for i, (side, to) in enumerate(
            [(-1, left), (1, right)] + list(zip((-1, 1, -1, 1), diagonals))
        )
    ]

    for c in early:
        c.wait()

    lane = lax.broadcasted_iota(jnp.int32, (1, C), 1)
    head_of = lane // HEAD
    heads = [(head_of == h).astype(F32).astype(BF) for h in range(HEADS)]

    entries = tbl.shape[-1]

    def lookup(index, side, b, h):
        line = tbl[side, b, h : h + 1, :]
        a0 = jnp.broadcast_to(line[:, 0:128], index.shape)
        a1 = jnp.concatenate([line[:, 128:], jnp.zeros((1, 256 - entries), F32)], axis=1)
        a1 = jnp.broadcast_to(a1, index.shape)
        within = jnp.bitwise_and(index, 127)
        g0 = jnp.take_along_axis(a0, within, axis=1)
        g1 = jnp.take_along_axis(a1, within, axis=1)
        return jnp.where(index < 128, g0, g1) * LOG2E

    def first_bias(side):
        twice = jnp.concatenate([rel[...], rel[...]], axis=1)
        for h in range(2):
            bias0[side, 64 * h : 64 * h + 64] = lookup(twice, side, 0, h)

    def zero_padded(values, side):
        pad = jnp.zeros_like(values)
        return jnp.concatenate([values, pad] if side == 0 else [pad, values], axis=1)

    first_bias(0)
    for m in range(3):
        bqkv[0, m : m + 1] = zero_padded(qkvb[0, m, 0:1], 0)

    def project(n, w, b):
        r = dot_rows(n, w[...].reshape(3 * C, C))
        q = ((r[:, 0:128] + bqkv[b, 0:1]) * QSCALE).astype(BF)
        k = (r[:, 128:256] + bqkv[b, 1:2]).astype(BF)
        v = (r[:, 256:384] + bqkv[b, 2:3]).astype(BF)
        return q, k, v

    ones = jnp.ones((64, C), BF)

    def weighted(s, values, each):
        raised = jnp.exp2(s - jnp.max(s, axis=1, keepdims=True)).astype(BF)
        o = dot(raised, jnp.concatenate([values, ones], axis=1))
        return [(o[i : i + each, 0:C], o[i : i + each, C:]) for i in range(0, s.shape[0], each)]

    def half_attention(side, q, k, v):
        stacked = jnp.concatenate([q * heads[2 * side], q * heads[2 * side + 1]], axis=0)
        s = dot_rows(stacked, k) + bias0[side, :, 0:64]
        (o0, l0), (o1, l1) = weighted(s, v, 64)
        here = head_of == 2 * side
        return (jnp.where(here, o0, o1) * (1.0 / jnp.where(here, l0, l1))).astype(BF)

    def windows_of(base):
        lines = [x[r, pl.ds(base, CHUNK), :].astype(F32) for r in range(WIN)]
        return jnp.concatenate(
            [lines[r][WIN * g : WIN * g + WIN] for g in range(GROUP) for r in range(WIN)], axis=0
        )

    def own_heads(j, carry):
        base = pl.multiple_of(j * CHUNK, CHUNK)
        at = pl.ds(pl.multiple_of(j * 64 * GROUP, 64 * GROUP), 64 * GROUP)
        n = norm(windows_of(base), gain[0, 0:1], shift[0, 0:1])
        normed[at, :] = n
        q, k, v = project(n, wown, 0)
        att[at, :] = jnp.concatenate(
            [half_attention(0, *(a[64 * g : 64 * g + 64] for a in (q, k, v))) for g in range(GROUP)],
            axis=0,
        )
        return carry

    lax.fori_loop(0, chunks, own_heads, 0)

    for c in late:
        c.wait()
    i = lax.broadcasted_iota(jnp.int32, lab.shape, 0)
    j = lax.broadcasted_iota(jnp.int32, lab.shape, 1)
    first_band = (band == 0).astype(jnp.int32)
    first_tile = (col == 0).astype(jnp.int32)
    region[...] = (
        lab[...] * 4
        + (i < SHIFT).astype(jnp.int32) * (2 * first_band)
        + (j < SHIFT).astype(jnp.int32) * first_tile
    )

    pl.semaphore_wait(barrier, len(peers))
    for c in first + second + region_copies + third:
        c.start()

    for c in first:
        c.wait_recv()
    first_bias(1)
    for m in range(3):
        bqkv[1, m : m + 1] = zero_padded(qkvb[1, m, 0:1], 1)
        bqkv[2, m : m + 1] = jnp.concatenate([qkvb[0, m, 1:2], qkvb[1, m, 1:2]], axis=1)
    for t, part in enumerate(
        (rel[0:32], jnp.concatenate([rel[32:64, 32:64], rel[32:64, 0:32]], axis=1))
    ):
        index = jnp.concatenate([part, part], axis=1)
        for h in range(HEADS):
            bias1[t, 32 * h : 32 * h + 32] = lookup(index, h // 2, 1, h % 2)

    def feed(b, attended, tokens):
        mid = (tokens + dot(attended, wproj[b]) + projb[b : b + 1]).astype(BF).astype(F32)
        n = norm(mid, gain[b, 1:2], shift[b, 1:2])
        total = mid + fc2b[b : b + 1]
        for side in range(2):
            inner = dot(n, w1[side, b]) + b1[side, b : b + 1]
            hidden = (inner * (0.5 + 0.5 * lax.erf(inner * ROOT_HALF))).astype(BF)
            total = total + dot(hidden, w2[side, b])
        return total.astype(BF).astype(F32)

    for c in second:
        c.wait_recv()

    def halo_copies(k):
        at = pl.ds(pl.multiple_of(k * CHUNK, CHUNK), CHUNK)
        return (
            copy(20 + k, halo.at[pl.ds(0, SHIFT), at], both.at[0, :, at], up),
            copy(24 + k, halo.at[pl.ds(SHIFT, SHIFT), at], both.at[1, :, at], down),
        )

    def first_block(k, carry):
        base = pl.multiple_of(k * CHUNK, CHUNK)
        at = pl.ds(pl.multiple_of(k * 64 * GROUP, 64 * GROUP), 64 * GROUP)
        q, key, v = project(normed[at, :], woth, 1)
        other = jnp.concatenate(
            [half_attention(1, *(a[64 * g : 64 * g + 64] for a in (q, key, v))) for g in range(GROUP)],
            axis=0,
        )
        done = feed(0, att[at, :] + other, windows_of(base))
        for r in range(WIN):
            line = jnp.concatenate(
                [done[64 * g + 8 * r : 64 * g + 8 * r + 8] for g in range(GROUP)], axis=0
            )
            y[SHIFT + r, pl.ds(base + SHIFT, CHUNK), :] = line
            halo[r, pl.ds(base, CHUNK), :] = line.astype(BF)
        for c in halo_copies(k):
            c.start()
        return carry

    lax.fori_loop(0, chunks, first_block, 0)

    edge = {-1: pl.ds(0, 16), 1: pl.ds(cols - 16, 16)}
    edge_copies = [
        copy(28, halo.at[:, edge[-1]], sides.at[1], left),
        copy(29, halo.at[:, edge[1]], sides.at[0], right),
    ] + [
        copy(30 + i, halo.at[pl.ds(r0, SHIFT), edge[side]], corners.at[i], to)
        for i, ((r0, side), to) in enumerate(
            zip(((0, -1), (0, 1), (SHIFT, -1), (SHIFT, 1)), diagonals)
        )
    ]
    for c in edge_copies:
        c.start()

    for c in region_copies:
        c.wait_recv()

    def spread(line):
        return jnp.broadcast_to(line.astype(F32), (128, 128)).T

    for r in range(2 * WIN):
        if r < SHIFT:
            middle, before, after, at = labs.at[1], labs.at[7], labs.at[6], SHIFT + r
        elif r < SHIFT + WIN:
            middle, before, after, at = region, labs.at[3], labs.at[2], r - SHIFT
        else:
            middle, before, after, at = labs.at[0], labs.at[5], labs.at[4], r - SHIFT - WIN
        for t in range(cols // 128):
            ids[r, SHIFT + 128 * t : SHIFT + 128 * t + 128, :] = spread(
                middle[at : at + 1, 128 * t : 128 * t + 128]
            )
        ids[r, 0:SHIFT, :] = spread(before[at : at + 1, 0:128])[128 - SHIFT :]
        ids[r, SHIFT + cols : 2 * SHIFT + cols, :] = spread(after[at : at + 1, 0:128])[0:SHIFT]

    for c in third:
        c.wait_recv()
    for c in edge_copies[0:2]:
        c.wait_recv()
    ends = ((slice(0, SHIFT), slice(12, 16)), (slice(SHIFT + cols, 2 * SHIFT + cols), slice(0, SHIFT)))
    for s, (to, of) in enumerate(ends):
        for r in range(WIN):
            y[SHIFT + r, to, :] = sides[s, r].astype(F32)[of]

    def shifted_band(is_bottom):
        mine = SHIFT + SHIFT * is_bottom
        theirs = (SHIFT + WIN) * is_bottom

        arrived = both.at[1 - is_bottom]
        flow = 20 + 4 * (1 - is_bottom)

        def take(k):
            at = pl.ds(pl.multiple_of(k * CHUNK, CHUNK), CHUNK)
            copy(flow + k, arrived.at[:, at], arrived.at[:, at], up).wait_recv()
            for r in range(SHIFT):
                y[theirs + r, pl.ds(k * CHUNK + SHIFT, CHUNK), :] = arrived[r, at, :].astype(F32)

        corner = 2 * (1 - is_bottom)
        for i in range(2):
            part = corners.at[corner + i]
            copy(30 + corner + i, part, part, up).wait_recv()
            to, of = ends[1 - i]
            for r in range(SHIFT):
                y[theirs + r, to, :] = part[r].astype(F32)[of]
        take(0)

        def body(c, carry):
            take(c + 1)
            base = pl.multiple_of(c * span * WIN, WIN)

            def gather(ref, row):
                return [
                    [ref[row + r, pl.ds(base + WIN * g, WIN), :] for r in range(SHIFT)]
                    for g in range(span)
                ]

            own = gather(y, mine)
            beside = gather(y, theirs)
            own_id = gather(ids, mine)
            beside_id = gather(ids, theirs)
            flat = lambda parts: jnp.concatenate([p for g in parts for p in g], axis=0)
            tokens = flat(own)
            n = norm(tokens, gain[1, 0:1], shift[1, 0:1])
            n2 = norm(flat(beside), gain[1, 0:1], shift[1, 0:1])
            q, k, v = project(n, wfull, 2)
            r2 = dot_rows(n2, wfull[1:3].reshape(2 * C, C))
            k2 = (r2[:, 0:128] + bqkv[2, 1:2]).astype(BF)
            v2 = (r2[:, 128:256] + bqkv[2, 2:3]).astype(BF)
            attended = []
            for g in range(span):
                at = slice(32 * g, 32 * g + 32)
                keys = jnp.concatenate([k[at], k2[at]], axis=0)
                values = jnp.concatenate([v[at], v2[at]], axis=0)
                stacked = jnp.concatenate([q[at] * m for m in heads], axis=0)
                s = dot_rows(stacked, keys) + bias1[1 - is_bottom, :, 0:64]
                key_id = jnp.concatenate(own_id[g] + beside_id[g], axis=0).T[0:8]
                allowed = jnp.concatenate([i[:, 0:64] == key_id for i in own_id[g]] * 4, axis=0)
                parts = weighted(jnp.where(allowed, s, EXCLUDED), values, 32)
                mixed, total = parts[3]
                for h in (2, 1, 0):
                    mixed = jnp.where(head_of == h, parts[h][0], mixed)
                    total = jnp.where(head_of == h, parts[h][1], total)
                mixed = mixed * (1.0 / total)
                attended.append(mixed.astype(BF))
            done = feed(1, jnp.concatenate(attended, axis=0), tokens)
            for g in range(span):
                for r in range(SHIFT):
                    i = 32 * g + 8 * r
                    y[mine + r, pl.ds(base + WIN * g, WIN), :] = done[i : i + 8]
            return carry

        lax.fori_loop(0, SPANS, body, 0)
        row = SHIFT * is_bottom
        for r in range(SHIFT):
            result[row + r] = y[mine + r, SHIFT : SHIFT + cols, :].astype(BF)
        return pltpu.make_async_copy(
            result.at[pl.ds(row, SHIFT)], out_ref.at[pl.ds(row, SHIFT)], local.at[15 + is_bottom]
        )

    near = 1 - ch
    outs = []
    for is_bottom in (near, 1 - near):
        c = shifted_band(is_bottom)
        c.start()
        outs.append(c)
    for c in outs:
        c.wait()

    for c in first + second + third + region_copies + edge_copies:
        c.wait_send()
    for k in range(chunks):
        for c in halo_copies(k):
            c.wait_send()


def on_device(
    image_tokens, labels, rel_index, norm_gain, norm_shift, qkv_weight, qkv_bias, bias_table,
    proj_weight, proj_bias, fc1_weight, fc1_bias, fc2_weight, fc2_bias,
):
    rows, cols, _ = image_tokens.shape
    args = (
        image_tokens, labels, rel_index, norm_gain, norm_shift,
        jnp.swapaxes(qkv_weight, 2, 3), jnp.swapaxes(qkv_bias, 0, 1),
        jnp.swapaxes(bias_table, 1, 2),
        proj_weight, proj_bias, fc1_weight, fc1_bias, fc2_weight, fc2_bias,
    )
    V = pltpu.VMEM
    like = lambda a, *lead: V((*lead, *a.shape), a.dtype)
    copies = 34
    return pl.pallas_call(
        kernel,
        out_shape=jax.ShapeDtypeStruct((rows, cols, C), BF),
        in_specs=[pl.BlockSpec(memory_space=pl.ANY)] * len(args),
        out_specs=pl.BlockSpec(memory_space=pl.ANY),
        scratch_shapes=[
            like(image_tokens), like(labels), like(rel_index), like(norm_gain), like(norm_shift),
            like(args[6], 2), like(args[7], 2),
            V((2, C, C), BF), like(proj_bias),
            like(fc1_weight, 2), like(fc1_bias, 2), like(fc2_weight, 2), like(fc2_bias),
            V((3, C, C), BF), V((3, C, C), BF), V((3, C, C), BF),
            V((3, 3, C), F32),
            V((2, C, C), F32), V((2, C, C), F32),
            V((2 * WIN, cols + 8, C), F32), V((2 * WIN, cols + 8, C), F32),
            V((rows * cols, C), BF), V((rows * cols, C), BF),
            V((rows, cols, C), BF),
            like(labels), like(labels, 8),
            V((rows, cols, C), BF), V((2, SHIFT, cols, C), BF),
            V((2, rows, 16, C), BF), V((4, SHIFT, 16, C), BF),
            pltpu.SemaphoreType.DMA((17,)),
            pltpu.SemaphoreType.DMA((copies,)),
            pltpu.SemaphoreType.DMA((copies,)),
        ],
        compiler_params=pltpu.CompilerParams(
            collective_id=0, has_side_effects=True, vmem_limit_bytes=60 * 1024 * 1024
        ),
        name="swin_pair",
    )(*args)


def solution(mesh):
    in_specs = (
        P(("row", "ch"), "col", None),
        P(("row", "ch"), "col"),
        P(),
        P(),
        P(),
        P(None, None, None, "ch"),
        P(None, None, "ch"),
        P(None, None, "ch"),
        P(None, "ch", None),
        P(),
        P(None, None, "ch"),
        P(None, "ch"),
        P(None, "ch", None),
        P(),
    )
    out_specs = P(("row", "ch"), "col", None)
    return jax.shard_map(
        on_device, mesh=mesh, in_specs=in_specs, out_specs=out_specs, check_vma=False
    )
```

```python
import functools
import math

import jax
import jax.numpy as jnp
from jax import lax
from jax.experimental import pallas as pl
from jax.experimental.pallas import tpu as pltpu
from jax.sharding import PartitionSpec as P

WIN = 8
SHIFT = 4
HEADS = 4
EPS = 1e-05
C = 128
HEAD = 32
BF = jnp.bfloat16
F32 = jnp.float32
LOG2E = math.log2(math.e)
QSCALE = LOG2E / math.sqrt(HEAD)
ROOT_HALF = math.sqrt(0.5)
EXCLUDED = -1e30
MESH = pl.DeviceIdType.MESH

GROUP = 8
CHUNK = GROUP * WIN
PACK = 2
SPANS = 3


def norm(x, gain, shift):
    center = x - jnp.mean(x, axis=-1, keepdims=True)
    spread = jnp.mean(center * center, axis=-1, keepdims=True)
    return (center * lax.rsqrt(spread + EPS) * gain + shift).astype(BF)


def dot(a, b):
    return jnp.dot(a, b, preferred_element_type=F32)


def dot_rows(a, b):
    return lax.dot_general(a, b, (((1,), (1,)), ((), ())), preferred_element_type=F32)


def kernel(
    x_in, lab_in, rel_in, gain_in, shift_in, qkvw_in, qkvb_in, tbl_in, projw_in,
    projb_in, fc1w_in, fc1b_in, fc2w_in, fc2b_in,
    out_ref,
    x, lab, rel, gain, shift, qkvb, tbl, wproj, projb, w1, b1, w2, fc2b,
    wown, woth, wfull, bqkv, bias0, bias1,
    y, ids, normed, att, result, region, labs,
    halo, both, sides, corners,
    local, send, recv,
):
    cols = x.shape[1]
    chunks = cols // CHUNK
    wins = cols // WIN + 1
    span = wins // SPANS
    groups = lax.axis_size("ch")
    bands = lax.axis_size("row") * groups
    tiles = lax.axis_size("col")
    ch = lax.axis_index("ch")
    col = lax.axis_index("col")
    band = lax.axis_index("row") * groups + ch

    def device(band_step, col_step):
        b = lax.rem(band + bands + band_step, bands)
        c = lax.rem(col + tiles + col_step, tiles)
        return {"row": b // groups, "col": c, "ch": lax.rem(b, groups)}

    partner = {"row": lax.axis_index("row"), "col": col, "ch": 1 - ch}
    across = {"row": lax.axis_index("row"), "col": lax.rem(col + tiles // 2, tiles), "ch": 1 - ch}
    up, down = device(-1, 0), device(1, 0)
    left, right = device(0, -1), device(0, 1)
    diagonals = [device(i, j) for i in (-1, 1) for j in (-1, 1)]

    barrier = pltpu.get_barrier_semaphore()
    peers = [up, down, left, right, across] + diagonals
    for peer in peers:
        pl.semaphore_signal(barrier, inc=1, device_id=peer, device_id_type=MESH)

    def load(i, src, dst):
        return pltpu.make_async_copy(src, dst, local.at[i])

    own_rows = pl.ds(0, 64)
    other_rows = pl.ds(64, 64)
    early = [
        load(0, x_in, x),
        load(1, qkvw_in.at[0], wown.at[:, own_rows]),
        load(2, qkvb_in, qkvb.at[0]),
        load(3, tbl_in, tbl.at[0]),
        load(4, rel_in, rel),
        load(5, gain_in, gain),
        load(6, shift_in, shift),
    ]
    late = [
        load(7, projw_in, wproj.at[:, own_rows]),
        load(8, fc1w_in, w1.at[0]),
        load(9, fc1b_in, b1.at[0]),
        load(10, fc2w_in, w2.at[0]),
        load(11, qkvw_in.at[1], wfull.at[:, own_rows]),
        load(12, projb_in, projb),
        load(13, fc2b_in, fc2b),
        load(14, lab_in, lab),
    ]
    for c in early + late:
        c.start()

    wown[:, 64:128, :] = jnp.zeros((3, 64, C), BF)
    woth[:, 0:64, :] = jnp.zeros((3, 64, C), BF)

    def copy(i, src, dst, to):
        return pltpu.make_async_remote_copy(
            src_ref=src, dst_ref=dst, send_sem=send.at[i], recv_sem=recv.at[i],
            device_id=to, device_id_type=MESH,
        )

    first = [
        copy(0, wown.at[:, own_rows], woth.at[:, other_rows], partner),
        copy(1, qkvb.at[0], qkvb.at[1], partner),
        copy(2, tbl.at[0], tbl.at[1], partner),
        copy(3, b1.at[0], b1.at[1], partner),
    ]
    def feed_copies(b):
        return [
            copy(4 + 4 * b, wproj.at[b, own_rows], wproj.at[b, other_rows], across),
            copy(5 + 4 * b, w1.at[0, b], w1.at[1, b], across),
            copy(6 + 4 * b, w2.at[0, b], w2.at[1, b], across),
        ]
    second = feed_copies(0)
    third = [copy(7, wfull.at[:, own_rows], wfull.at[:, other_rows], across)] + feed_copies(1)
    half_at = {-1: pl.ds(0, 128), 1: pl.ds(cols - 128, 128)}
    region_copies = [
        copy(11, region.at[pl.ds(0, SHIFT)], labs.at[0, pl.ds(0, SHIFT)], up),
        copy(12, region.at[pl.ds(SHIFT, SHIFT)], labs.at[1, pl.ds(SHIFT, SHIFT)], down),
        copy(13, region.at[:, half_at[-1]], labs.at[2, :, pl.ds(0, 128)], left),
        copy(14, region.at[:, half_at[1]], labs.at[3, :, pl.ds(0, 128)], right),
    ] + [
        copy(
            15 + i, region.at[pl.ds(r0, SHIFT), half_at[side]],
            labs.at[4 + i, pl.ds(r0, SHIFT), pl.ds(0, 128)], to,
        )
        for i, ((r0, side), to) in enumerate(
            zip(((0, -1), (0, 1), (SHIFT, -1), (SHIFT, 1)), diagonals)
        )
    ]

    for c in early:
        c.wait()

    lane = lax.broadcasted_iota(jnp.int32, (1, C), 1)
    head_of = lane // HEAD
    heads = [(head_of == h).astype(F32).astype(BF) for h in range(HEADS)]

    entries = tbl.shape[-1]

    def lookup(index, side, b, h):
        line = tbl[side, b, h : h + 1, :]
        a0 = jnp.broadcast_to(line[:, 0:128], index.shape)
        a1 = jnp.concatenate([line[:, 128:], jnp.zeros((1, 256 - entries), F32)], axis=1)
        a1 = jnp.broadcast_to(a1, index.shape)
        within = jnp.bitwise_and(index, 127)
        g0 = jnp.take_along_axis(a0, within, axis=1)
        g1 = jnp.take_along_axis(a1, within, axis=1)
        return jnp.where(index < 128, g0, g1) * LOG2E

    def put_bias(bias, i, rows, values):
        bias[i, 0, rows] = jnp.where(lane < 64, values, EXCLUDED)
        bias[i, 1, rows] = jnp.where(lane < 64, EXCLUDED, values)

    def first_bias(side):
        twice = jnp.concatenate([rel[...], rel[...]], axis=1)
        for h in range(2):
            put_bias(bias0, side, slice(64 * h, 64 * h + 64), lookup(twice, side, 0, h))

    def zero_padded(values, side):
        pad = jnp.zeros_like(values)
        return jnp.concatenate([values, pad] if side == 0 else [pad, values], axis=1)

    first_bias(0)
    for m in range(3):
        bqkv[0, m : m + 1] = zero_padded(qkvb[0, m, 0:1], 0)

    def project(n, w, b):
        r = dot_rows(n, w[...].reshape(3 * C, C))
        q = ((r[:, 0:128] + bqkv[b, 0:1]) * QSCALE).astype(BF)
        k = (r[:, 128:256] + bqkv[b, 1:2]).astype(BF)
        v = (r[:, 256:384] + bqkv[b, 2:3]).astype(BF)
        return q, k, v

    def weighted(queries, keys, values, bias, allowed, each):
        width = 64 * len(queries)
        s = dot_rows(jnp.concatenate(queries, axis=0), jnp.concatenate(keys, axis=0))
        s = [s[C * i : C * i + C] + bias[i, :, 0:width] for i in range(len(queries))]
        if allowed is not None:
            s = [jnp.where(a, b, EXCLUDED) for a, b in zip(allowed, s)]
        raised = [jnp.exp2(a - jnp.max(a, axis=1, keepdims=True)) for a in s]
        totals = [jnp.sum(a, axis=1, keepdims=True) for a in raised]
        o = dot(
            jnp.concatenate([a.astype(BF) for a in raised], axis=0),
            jnp.concatenate(values, axis=0),
        )
        mixed = []
        for i, total in enumerate(totals):
            part = o[C * i : C * i + C] * (1.0 / total)
            mixed.append([part[k : k + each] for k in range(0, C, each)])
        return mixed

    def half_attention(side, q, k, v):
        cut = lambda a: [a[64 * g : 64 * g + 64] for g in range(GROUP)]
        stacked = [
            jnp.concatenate([a * heads[2 * side], a * heads[2 * side + 1]], axis=0) for a in cut(q)
        ]
        k, v = cut(k), cut(v)
        out = []
        for g in range(0, GROUP, 2):
            two = slice(g, g + 2)
            for o0, o1 in weighted(stacked[two], k[two], v[two], bias0.at[side], None, 64):
                out.append(jnp.where(head_of == 2 * side, o0, o1).astype(BF))
        return jnp.concatenate(out, axis=0)

    def windows_of(base):
        lines = [x[r, pl.ds(base, CHUNK), :].astype(F32) for r in range(WIN)]
        return jnp.concatenate(
            [lines[r][WIN * g : WIN * g + WIN] for g in range(GROUP) for r in range(WIN)], axis=0
        )

    def own_heads(j, carry):
        base = pl.multiple_of(j * CHUNK, CHUNK)
        at = pl.ds(pl.multiple_of(j * 64 * GROUP, 64 * GROUP), 64 * GROUP)
        n = norm(windows_of(base), gain[0, 0:1], shift[0, 0:1])
        normed[at, :] = n
        q, k, v = project(n, wown, 0)
        att[at, :] = half_attention(0, q, k, v)
        return carry

    lax.fori_loop(0, chunks, own_heads, 0)

    for c in late:
        c.wait()
    i = lax.broadcasted_iota(jnp.int32, lab.shape, 0)
    j = lax.broadcasted_iota(jnp.int32, lab.shape, 1)
    first_band = (band == 0).astype(jnp.int32)
    first_tile = (col == 0).astype(jnp.int32)
    region[...] = (
        lab[...] * 4
        + (i < SHIFT).astype(jnp.int32) * (2 * first_band)
        + (j < SHIFT).astype(jnp.int32) * first_tile
    )

    pl.semaphore_wait(barrier, len(peers))
    for c in first + second + region_copies + third:
        c.start()

    for c in first:
        c.wait_recv()
    first_bias(1)
    for m in range(3):
        bqkv[1, m : m + 1] = zero_padded(qkvb[1, m, 0:1], 1)
        bqkv[2, m : m + 1] = jnp.concatenate([qkvb[0, m, 1:2], qkvb[1, m, 1:2]], axis=1)
    for t, part in enumerate(
        (rel[0:32], jnp.concatenate([rel[32:64, 32:64], rel[32:64, 0:32]], axis=1))
    ):
        index = jnp.concatenate([part, part], axis=1)
        for h in range(HEADS):
            put_bias(bias1, t, slice(32 * h, 32 * h + 32), lookup(index, h // 2, 1, h % 2))

    def feed(b, attended, tokens):
        mid = (tokens + dot(attended, wproj[b]) + projb[b : b + 1]).astype(BF).astype(F32)
        n = norm(mid, gain[b, 1:2], shift[b, 1:2])
        total = mid + fc2b[b : b + 1]
        for side in range(2):
            inner = dot(n, w1[side, b]) + b1[side, b : b + 1]
            hidden = (inner * (0.5 + 0.5 * lax.erf(inner * ROOT_HALF))).astype(BF)
            total = total + dot(hidden, w2[side, b])
        return total.astype(BF).astype(F32)

    for c in second:
        c.wait_recv()

    def halo_copy(near, k):
        at = pl.ds(pl.multiple_of(k * CHUNK, CHUNK), CHUNK)
        to_down = 1 - ch if near else ch
        return copy(
            20 + 4 * to_down + k, halo.at[pl.ds(SHIFT * to_down, SHIFT), at],
            both.at[to_down, :, at], partner if near else device(2 * ch - 1, 0),
        )

    def first_block(k, carry):
        base = pl.multiple_of(k * CHUNK, CHUNK)
        at = pl.ds(pl.multiple_of(k * 64 * GROUP, 64 * GROUP), 64 * GROUP)
        q, key, v = project(normed[at, :], woth, 1)
        other = half_attention(1, q, key, v)
        done = feed(0, att[at, :] + other, windows_of(base))
        for r in range(WIN):
            line = jnp.concatenate(
                [done[64 * g + 8 * r : 64 * g + 8 * r + 8] for g in range(GROUP)], axis=0
            )
            y[SHIFT + r, pl.ds(base + SHIFT, CHUNK), :] = line
            halo[r, pl.ds(base, CHUNK), :] = line.astype(BF)
        halo_copy(True, k).start()
        return carry

    lax.fori_loop(0, chunks, first_block, 0)

    for k in range(chunks):
        halo_copy(False, k).start()
    edge = {-1: pl.ds(0, 16), 1: pl.ds(cols - 16, 16)}
    edge_copies = [
        copy(28, halo.at[:, edge[-1]], sides.at[1], left),
        copy(29, halo.at[:, edge[1]], sides.at[0], right),
    ] + [
        copy(30 + i, halo.at[pl.ds(r0, SHIFT), edge[side]], corners.at[i], to)
        for i, ((r0, side), to) in enumerate(
            zip(((0, -1), (0, 1), (SHIFT, -1), (SHIFT, 1)), diagonals)
        )
    ]
    for c in edge_copies:
        c.start()

    for c in region_copies:
        c.wait_recv()

    def spread(line):
        return jnp.broadcast_to(line.astype(F32), (128, 128)).T

    for r in range(2 * WIN):
        if r < SHIFT:
            middle, before, after, at = labs.at[1], labs.at[7], labs.at[6], SHIFT + r
        elif r < SHIFT + WIN:
            middle, before, after, at = region, labs.at[3], labs.at[2], r - SHIFT
        else:
            middle, before, after, at = labs.at[0], labs.at[5], labs.at[4], r - SHIFT - WIN
        for t in range(cols // 128):
            ids[r, SHIFT + 128 * t : SHIFT + 128 * t + 128, :] = spread(
                middle[at : at + 1, 128 * t : 128 * t + 128]
            )
        ids[r, 0:SHIFT, :] = spread(before[at : at + 1, 0:128])[128 - SHIFT :]
        ids[r, SHIFT + cols : 2 * SHIFT + cols, :] = spread(after[at : at + 1, 0:128])[0:SHIFT]

    for c in third:
        c.wait_recv()
    for c in edge_copies[0:2]:
        c.wait_recv()
    ends = ((slice(0, SHIFT), slice(12, 16)), (slice(SHIFT + cols, 2 * SHIFT + cols), slice(0, SHIFT)))
    for s, (to, of) in enumerate(ends):
        for r in range(WIN):
            y[SHIFT + r, to, :] = sides[s, r].astype(F32)[of]

    def shifted_band(is_bottom):
        mine = SHIFT + SHIFT * is_bottom
        theirs = (SHIFT + WIN) * is_bottom

        arrived = both.at[1 - is_bottom]
        flow = 20 + 4 * (1 - is_bottom)

        def take(k):
            at = pl.ds(pl.multiple_of(k * CHUNK, CHUNK), CHUNK)
            copy(flow + k, arrived.at[:, at], arrived.at[:, at], up).wait_recv()
            for r in range(SHIFT):
                y[theirs + r, pl.ds(k * CHUNK + SHIFT, CHUNK), :] = arrived[r, at, :].astype(F32)

        corner = 2 * (1 - is_bottom)
        for i in range(2):
            part = corners.at[corner + i]
            copy(30 + corner + i, part, part, up).wait_recv()
            to, of = ends[1 - i]
            for r in range(SHIFT):
                y[theirs + r, to, :] = part[r].astype(F32)[of]
        take(0)

        def body(c, carry):
            take(c + 1)
            base = pl.multiple_of(c * span * WIN, WIN)

            def gather(ref, row):
                return [
                    [ref[row + r, pl.ds(base + WIN * g, WIN), :] for r in range(SHIFT)]
                    for g in range(span)
                ]

            own = gather(y, mine)
            beside = gather(y, theirs)
            own_id = gather(ids, mine)
            beside_id = gather(ids, theirs)
            flat = lambda parts: jnp.concatenate([p for g in parts for p in g], axis=0)
            tokens = flat(own)
            n = norm(tokens, gain[1, 0:1], shift[1, 0:1])
            n2 = norm(flat(beside), gain[1, 0:1], shift[1, 0:1])
            q, k, v = project(n, wfull, 2)
            r2 = dot_rows(n2, wfull[1:3].reshape(2 * C, C))
            k2 = (r2[:, 0:128] + bqkv[2, 1:2]).astype(BF)
            v2 = (r2[:, 128:256] + bqkv[2, 2:3]).astype(BF)
            attended = []
            for first_window in range(0, span, PACK):
                group = [min(first_window + i, span - 1) for i in range(PACK)]
                queries, keys, values, key_ids = [], [], [], []
                for g in group:
                    at = slice(32 * g, 32 * g + 32)
                    queries.append(jnp.concatenate([q[at] * m for m in heads], axis=0))
                    keys.append(jnp.concatenate([k[at], k2[at]], axis=0))
                    values.append(jnp.concatenate([v[at], v2[at]], axis=0))
                    key_ids += own_id[g] + beside_id[g]
                key_id = jnp.concatenate(key_ids, axis=0).T[0:8]
                width = 64 * len(group)
                allowed = [
                    jnp.concatenate([i[:, 0:width] == key_id for i in own_id[g]] * 4, axis=0)
                    for g in group
                ]
                for parts in weighted(queries, keys, values, bias1.at[1 - is_bottom], allowed, 32)[: span - first_window]:
                    mixed = parts[3]
                    for h in (2, 1, 0):
                        mixed = jnp.where(head_of == h, parts[h], mixed)
                    attended.append(mixed.astype(BF))
            done = feed(1, jnp.concatenate(attended, axis=0), tokens)
            for g in range(span):
                for r in range(SHIFT):
                    i = 32 * g + 8 * r
                    y[mine + r, pl.ds(base + WIN * g, WIN), :] = done[i : i + 8]
            return carry

        lax.fori_loop(0, SPANS, body, 0)
        row = SHIFT * is_bottom
        for r in range(SHIFT):
            result[row + r] = y[mine + r, SHIFT : SHIFT + cols, :].astype(BF)
        return pltpu.make_async_copy(
            result.at[pl.ds(row, SHIFT)], out_ref.at[pl.ds(row, SHIFT)], local.at[15 + is_bottom]
        )

    near = 1 - ch
    outs = []
    for is_bottom in (near, 1 - near):
        c = shifted_band(is_bottom)
        c.start()
        outs.append(c)
    for c in outs:
        c.wait()

    for c in first + second + third + region_copies + edge_copies:
        c.wait_send()
    for k in range(chunks):
        for near in (True, False):
            halo_copy(near, k).wait_send()


def on_device(
    image_tokens, labels, rel_index, norm_gain, norm_shift, qkv_weight, qkv_bias, bias_table,
    proj_weight, proj_bias, fc1_weight, fc1_bias, fc2_weight, fc2_bias,
):
    rows, cols, _ = image_tokens.shape
    args = (
        image_tokens, labels, rel_index, norm_gain, norm_shift,
        jnp.swapaxes(qkv_weight, 2, 3), jnp.swapaxes(qkv_bias, 0, 1),
        jnp.swapaxes(bias_table, 1, 2),
        proj_weight, proj_bias, fc1_weight, fc1_bias, fc2_weight, fc2_bias,
    )
    V = pltpu.VMEM
    like = lambda a, *lead: V((*lead, *a.shape), a.dtype)
    copies = 34
    return pl.pallas_call(
        kernel,
        out_shape=jax.ShapeDtypeStruct((rows, cols, C), BF),
        in_specs=[pl.BlockSpec(memory_space=pl.ANY)] * len(args),
        out_specs=pl.BlockSpec(memory_space=pl.ANY),
        scratch_shapes=[
            like(image_tokens), like(labels), like(rel_index), like(norm_gain), like(norm_shift),
            like(args[6], 2), like(args[7], 2),
            V((2, C, C), BF), like(proj_bias),
            like(fc1_weight, 2), like(fc1_bias, 2), like(fc2_weight, 2), like(fc2_bias),
            V((3, C, C), BF), V((3, C, C), BF), V((3, C, C), BF),
            V((3, 3, C), F32),
            V((2, PACK, C, C), F32), V((2, PACK, C, C), F32),
            V((2 * WIN, cols + 8, C), F32), V((2 * WIN, cols + 8, C), F32),
            V((rows * cols, C), BF), V((rows * cols, C), BF),
            V((rows, cols, C), BF),
            like(labels), like(labels, 8),
            V((rows, cols, C), BF), V((2, SHIFT, cols, C), BF),
            V((2, rows, 16, C), BF), V((4, SHIFT, 16, C), BF),
            pltpu.SemaphoreType.DMA((17,)),
            pltpu.SemaphoreType.DMA((copies,)),
            pltpu.SemaphoreType.DMA((copies,)),
        ],
        compiler_params=pltpu.CompilerParams(
            collective_id=0, has_side_effects=True, vmem_limit_bytes=60 * 1024 * 1024
        ),
        name="swin_pair",
    )(*args)


def solution(mesh):
    in_specs = (
        P(("row", "ch"), "col", None),
        P(("row", "ch"), "col"),
        P(),
        P(),
        P(),
        P(None, None, None, "ch"),
        P(None, None, "ch"),
        P(None, None, "ch"),
        P(None, "ch", None),
        P(),
        P(None, None, "ch"),
        P(None, "ch"),
        P(None, "ch", None),
        P(),
    )
    out_specs = P(("row", "ch"), "col", None)
    return jax.shard_map(
        on_device, mesh=mesh, in_specs=in_specs, out_specs=out_specs, check_vma=False
    )
```

```python
import functools
import math

import jax
import jax.numpy as jnp
from jax import lax
from jax.experimental import pallas as pl
from jax.experimental.pallas import tpu as pltpu
from jax.sharding import PartitionSpec as P

WIN = 8
SHIFT = 4
HEADS = 4
EPS = 1e-05
C = 128
HEAD = 32
BF = jnp.bfloat16
F32 = jnp.float32
LOG2E = math.log2(math.e)
QSCALE = LOG2E / math.sqrt(HEAD)
ROOT_HALF = math.sqrt(0.5)
EXCLUDED = -1e30
MESH = pl.DeviceIdType.MESH

GROUP = 8
CHUNK = GROUP * WIN
PACK = 2
SPANS = 3


def norm(x, gain, shift):
    center = x - jnp.mean(x, axis=-1, keepdims=True)
    spread = jnp.mean(center * center, axis=-1, keepdims=True)
    return (center * lax.rsqrt(spread + EPS) * gain + shift).astype(BF)


def dot(a, b):
    return jnp.dot(a, b, preferred_element_type=F32)


def dot_rows(a, b):
    return lax.dot_general(a, b, (((1,), (1,)), ((), ())), preferred_element_type=F32)


def kernel(
    x_in, lab_in, rel_in, gain_in, shift_in, qkvw_in, qkvb_in, tbl_in, projw_in,
    projb_in, fc1w_in, fc1b_in, fc2w_in, fc2b_in,
    out_ref,
    x, lab, rel, gain, shift, qkvb, tbl, wproj, projb, w1, b1, w2, fc2b,
    wown, woth, wfull, bqkv, bias0, bias1,
    y, ids, normed, att, region, labs,
    halo, both, sides, corners,
    local, send, recv,
):
    cols = x.shape[1]
    chunks = cols // CHUNK
    wins = cols // WIN + 1
    span = wins // SPANS
    groups = lax.axis_size("ch")
    bands = lax.axis_size("row") * groups
    tiles = lax.axis_size("col")
    ch = lax.axis_index("ch")
    col = lax.axis_index("col")
    band = lax.axis_index("row") * groups + ch

    def device(band_step, col_step):
        b = lax.rem(band + bands + band_step, bands)
        c = lax.rem(col + tiles + col_step, tiles)
        return {"row": b // groups, "col": c, "ch": lax.rem(b, groups)}

    partner = {"row": lax.axis_index("row"), "col": col, "ch": 1 - ch}
    across = {"row": lax.axis_index("row"), "col": lax.rem(col + tiles // 2, tiles), "ch": 1 - ch}
    up, down = device(-1, 0), device(1, 0)
    left, right = device(0, -1), device(0, 1)
    diagonals = [device(i, j) for i in (-1, 1) for j in (-1, 1)]

    barrier = pltpu.get_barrier_semaphore()
    peers = [up, down, left, right, across] + diagonals
    for peer in peers:
        pl.semaphore_signal(barrier, inc=1, device_id=peer, device_id_type=MESH)

    def load(i, src, dst):
        return pltpu.make_async_copy(src, dst, local.at[i])

    own_rows = pl.ds(0, 64)
    other_rows = pl.ds(64, 64)
    early = [
        load(0, x_in, x),
        load(1, qkvw_in.at[0], wown.at[:, own_rows]),
        load(2, qkvb_in, qkvb.at[0]),
        load(3, tbl_in, tbl.at[0]),
        load(4, rel_in, rel),
        load(5, gain_in, gain),
        load(6, shift_in, shift),
    ]
    late = [
        load(7, projw_in, wproj.at[:, own_rows]),
        load(8, fc1w_in, w1.at[0]),
        load(9, fc1b_in, b1.at[0]),
        load(10, fc2w_in, w2.at[0]),
        load(11, qkvw_in.at[1], wfull.at[:, own_rows]),
        load(12, projb_in, projb),
        load(13, fc2b_in, fc2b),
        load(14, lab_in, lab),
    ]
    for c in early + late:
        c.start()

    wown[:, 64:128, :] = jnp.zeros((3, 64, C), BF)
    woth[:, 0:64, :] = jnp.zeros((3, 64, C), BF)

    def copy(i, src, dst, to):
        return pltpu.make_async_remote_copy(
            src_ref=src, dst_ref=dst, send_sem=send.at[i], recv_sem=recv.at[i],
            device_id=to, device_id_type=MESH,
        )

    first = [
        copy(0, wown.at[:, own_rows], woth.at[:, other_rows], partner),
        copy(1, qkvb.at[0], qkvb.at[1], partner),
        copy(2, tbl.at[0], tbl.at[1], partner),
        copy(3, b1.at[0], b1.at[1], partner),
    ]
    def feed_copies(b):
        return [
            copy(4 + 4 * b, wproj.at[b, own_rows], wproj.at[b, other_rows], across),
            copy(5 + 4 * b, w1.at[0, b], w1.at[1, b], (partner, across)[b]),
            copy(6 + 4 * b, w2.at[0, b], w2.at[1, b], across),
        ]
    second = feed_copies(0)
    third = [copy(7, wfull.at[:, own_rows], wfull.at[:, other_rows], across)] + feed_copies(1)
    half_at = {-1: pl.ds(0, 128), 1: pl.ds(cols - 128, 128)}
    region_copies = [
        copy(11, region.at[pl.ds(0, SHIFT)], labs.at[0, pl.ds(0, SHIFT)], up),
        copy(12, region.at[pl.ds(SHIFT, SHIFT)], labs.at[1, pl.ds(SHIFT, SHIFT)], down),
        copy(13, region.at[:, half_at[-1]], labs.at[2, :, pl.ds(0, 128)], left),
        copy(14, region.at[:, half_at[1]], labs.at[3, :, pl.ds(0, 128)], right),
    ] + [
        copy(
            15 + i, region.at[pl.ds(r0, SHIFT), half_at[side]],
            labs.at[4 + i, pl.ds(r0, SHIFT), pl.ds(0, 128)], to,
        )
        for i, ((r0, side), to) in enumerate(
            zip(((0, -1), (0, 1), (SHIFT, -1), (SHIFT, 1)), diagonals)
        )
    ]

    for c in early:
        c.wait()

    lane = lax.broadcasted_iota(jnp.int32, (1, C), 1)
    head_of = lane // HEAD
    heads = [(head_of == h).astype(F32).astype(BF) for h in range(HEADS)]

    entries = tbl.shape[-1]

    def lookup(index, side, b, h):
        line = tbl[side, b, h : h + 1, :]
        a0 = jnp.broadcast_to(line[:, 0:128], index.shape)
        a1 = jnp.concatenate([line[:, 128:], jnp.zeros((1, 256 - entries), F32)], axis=1)
        a1 = jnp.broadcast_to(a1, index.shape)
        within = jnp.bitwise_and(index, 127)
        g0 = jnp.take_along_axis(a0, within, axis=1)
        g1 = jnp.take_along_axis(a1, within, axis=1)
        return jnp.where(index < 128, g0, g1) * LOG2E

    def put_bias(bias, i, rows, values):
        bias[i, 0, rows] = jnp.where(lane < 64, values, EXCLUDED)
        bias[i, 1, rows] = jnp.where(lane < 64, EXCLUDED, values)

    def first_bias(side):
        twice = jnp.concatenate([rel[...], rel[...]], axis=1)
        for h in range(2):
            put_bias(bias0, side, slice(64 * h, 64 * h + 64), lookup(twice, side, 0, h))

    def zero_padded(values, side):
        pad = jnp.zeros_like(values)
        return jnp.concatenate([values, pad] if side == 0 else [pad, values], axis=1)

    first_bias(0)
    for m in range(3):
        bqkv[0, m : m + 1] = zero_padded(qkvb[0, m, 0:1], 0)

    def project(n, w, b):
        r = dot_rows(n, w[...].reshape(3 * C, C))
        q = ((r[:, 0:128] + bqkv[b, 0:1]) * QSCALE).astype(BF)
        k = (r[:, 128:256] + bqkv[b, 1:2]).astype(BF)
        v = (r[:, 256:384] + bqkv[b, 2:3]).astype(BF)
        return q, k, v

    def weighted(queries, keys, values, bias, allowed, each):
        width = 64 * len(queries)
        s = dot_rows(jnp.concatenate(queries, axis=0), jnp.concatenate(keys, axis=0))
        s = [s[C * i : C * i + C] + bias[i, :, 0:width] for i in range(len(queries))]
        if allowed is not None:
            s = [jnp.where(a, b, EXCLUDED) for a, b in zip(allowed, s)]
        raised = [jnp.exp2(a - jnp.max(a, axis=1, keepdims=True)) for a in s]
        totals = [jnp.sum(a, axis=1, keepdims=True) for a in raised]
        o = dot(
            jnp.concatenate([a.astype(BF) for a in raised], axis=0),
            jnp.concatenate(values, axis=0),
        )
        mixed = []
        for i, total in enumerate(totals):
            part = o[C * i : C * i + C] * (1.0 / total)
            mixed.append([part[k : k + each] for k in range(0, C, each)])
        return mixed

    def half_attention(side, q, k, v):
        cut = lambda a: [a[64 * g : 64 * g + 64] for g in range(GROUP)]
        stacked = [
            jnp.concatenate([a * heads[2 * side], a * heads[2 * side + 1]], axis=0) for a in cut(q)
        ]
        k, v = cut(k), cut(v)
        out = []
        for g in range(0, GROUP, 2):
            two = slice(g, g + 2)
            for o0, o1 in weighted(stacked[two], k[two], v[two], bias0.at[side], None, 64):
                out.append(jnp.where(head_of == 2 * side, o0, o1).astype(BF))
        return jnp.concatenate(out, axis=0)

    def windows_of(base):
        lines = [x[r, pl.ds(base, CHUNK), :].astype(F32) for r in range(WIN)]
        return jnp.concatenate(
            [lines[r][WIN * g : WIN * g + WIN] for g in range(GROUP) for r in range(WIN)], axis=0
        )

    def meet():
        for c in late:
            c.wait()
        i = lax.broadcasted_iota(jnp.int32, lab.shape, 0)
        j = lax.broadcasted_iota(jnp.int32, lab.shape, 1)
        first_band = (band == 0).astype(jnp.int32)
        first_tile = (col == 0).astype(jnp.int32)
        region[...] = (
            lab[...] * 4
            + (i < SHIFT).astype(jnp.int32) * (2 * first_band)
            + (j < SHIFT).astype(jnp.int32) * first_tile
        )

        pl.semaphore_wait(barrier, len(peers))
        for c in first + second + third + region_copies:
            c.start()

    def own_heads(j, carry):
        pl.when(j == 1)(meet)
        base = pl.multiple_of(j * CHUNK, CHUNK)
        at = pl.ds(pl.multiple_of(j * 64 * GROUP, 64 * GROUP), 64 * GROUP)
        n = norm(windows_of(base), gain[0, 0:1], shift[0, 0:1])
        normed[at, :] = n
        q, k, v = project(n, wown, 0)
        att[at, :] = half_attention(0, q, k, v)
        return carry

    lax.fori_loop(0, chunks, own_heads, 0)

    for c in first:
        c.wait_recv()
    first_bias(1)
    for m in range(3):
        bqkv[1, m : m + 1] = zero_padded(qkvb[1, m, 0:1], 1)
        bqkv[2, m : m + 1] = jnp.concatenate([qkvb[0, m, 1:2], qkvb[1, m, 1:2]], axis=1)
    for t, part in enumerate(
        (rel[0:32], jnp.concatenate([rel[32:64, 32:64], rel[32:64, 0:32]], axis=1))
    ):
        index = jnp.concatenate([part, part], axis=1)
        for h in range(HEADS):
            put_bias(bias1, t, slice(32 * h, 32 * h + 32), lookup(index, h // 2, 1, h % 2))

    def feed(b, attended, tokens):
        mid = (tokens + dot(attended, wproj[b]) + projb[b : b + 1]).astype(BF).astype(F32)
        n = norm(mid, gain[b, 1:2], shift[b, 1:2])
        total = mid + fc2b[b : b + 1]
        for side in range(2):
            inner = dot(n, w1[side, b]) + b1[side, b : b + 1]
            hidden = (inner * (0.5 + 0.5 * lax.erf(inner * ROOT_HALF))).astype(BF)
            total = total + dot(hidden, w2[side, b])
        return total.astype(BF).astype(F32)

    for c in second:
        c.wait_recv()

    def halo_copy(near, k):
        at = pl.ds(pl.multiple_of(k * CHUNK, CHUNK), CHUNK)
        to_down = 1 - ch if near else ch
        return copy(
            20 + 4 * to_down + k, halo.at[pl.ds(SHIFT * to_down, SHIFT), at],
            both.at[to_down, :, at], partner if near else device(2 * ch - 1, 0),
        )

    edge = {-1: pl.ds(0, 16), 1: pl.ds(cols - 16, 16)}
    side_copies = [
        copy(28, halo.at[:, edge[-1]], sides.at[1], left),
        copy(29, halo.at[:, edge[1]], sides.at[0], right),
    ]

    def corner_copies(near):
        to_down = 1 - ch if near else ch
        return [
            copy(
                30 + 2 * to_down + i, halo.at[pl.ds(SHIFT * to_down, SHIFT), edge[side]],
                corners.at[2 * to_down + i], device(2 * to_down - 1, side),
            )
            for i, side in enumerate((-1, 1))
        ]

    def first_block(step, carry):
        k = lax.rem(step + chunks - 1, chunks)
        base = pl.multiple_of(k * CHUNK, CHUNK)
        at = pl.ds(pl.multiple_of(k * 64 * GROUP, 64 * GROUP), 64 * GROUP)
        q, key, v = project(normed[at, :], woth, 1)
        other = half_attention(1, q, key, v)
        done = feed(0, att[at, :] + other, windows_of(base))
        for r in range(WIN):
            line = jnp.concatenate(
                [done[64 * g + 8 * r : 64 * g + 8 * r + 8] for g in range(GROUP)], axis=0
            )
            y[SHIFT + r, pl.ds(base + SHIFT, CHUNK), :] = line
            halo[r, pl.ds(base, CHUNK), :] = line.astype(BF)
        halo_copy(True, k).start()

        @pl.when(step == 1)
        def _():
            for c in side_copies + corner_copies(True):
                c.start()

        return carry

    lax.fori_loop(0, chunks, first_block, 0)

    for k in range(chunks):
        halo_copy(False, k).start()
    for c in corner_copies(False):
        c.start()

    for c in region_copies:
        c.wait_recv()

    def spread(line):
        return jnp.broadcast_to(line.astype(F32), (128, 128)).T

    for r in range(2 * WIN):
        if r < SHIFT:
            middle, before, after, at = labs.at[1], labs.at[7], labs.at[6], SHIFT + r
        elif r < SHIFT + WIN:
            middle, before, after, at = region, labs.at[3], labs.at[2], r - SHIFT
        else:
            middle, before, after, at = labs.at[0], labs.at[5], labs.at[4], r - SHIFT - WIN
        for t in range(cols // 128):
            ids[r, SHIFT + 128 * t : SHIFT + 128 * t + 128, :] = spread(
                middle[at : at + 1, 128 * t : 128 * t + 128]
            )
        ids[r, 0:SHIFT, :] = spread(before[at : at + 1, 0:128])[128 - SHIFT :]
        ids[r, SHIFT + cols : 2 * SHIFT + cols, :] = spread(after[at : at + 1, 0:128])[0:SHIFT]

    for c in third:
        c.wait_recv()
    for c in side_copies:
        c.wait_recv()
    ends = ((slice(0, SHIFT), slice(12, 16)), (slice(SHIFT + cols, 2 * SHIFT + cols), slice(0, SHIFT)))
    for s, (to, of) in enumerate(ends):
        for r in range(WIN):
            y[SHIFT + r, to, :] = sides[s, r].astype(F32)[of]

    def shifted_band(is_bottom):
        mine = SHIFT + SHIFT * is_bottom
        theirs = (SHIFT + WIN) * is_bottom

        arrived = both.at[1 - is_bottom]
        flow = 20 + 4 * (1 - is_bottom)

        def take(k):
            at = pl.ds(pl.multiple_of(k * CHUNK, CHUNK), CHUNK)
            copy(flow + k, arrived.at[:, at], arrived.at[:, at], up).wait_recv()
            for r in range(SHIFT):
                y[theirs + r, pl.ds(k * CHUNK + SHIFT, CHUNK), :] = arrived[r, at, :].astype(F32)

        corner = 2 * (1 - is_bottom)
        for i in range(2):
            part = corners.at[corner + i]
            copy(30 + corner + i, part, part, up).wait_recv()
            to, of = ends[1 - i]
            for r in range(SHIFT):
                y[theirs + r, to, :] = part[r].astype(F32)[of]
        take(0)

        def body(c, carry):
            take(c + 1)
            base = pl.multiple_of(c * span * WIN, WIN)

            def gather(ref, row):
                return [
                    [ref[row + r, pl.ds(base + WIN * g, WIN), :] for r in range(SHIFT)]
                    for g in range(span)
                ]

            own = gather(y, mine)
            beside = gather(y, theirs)
            own_id = gather(ids, mine)
            beside_id = gather(ids, theirs)
            flat = lambda parts: jnp.concatenate([p for g in parts for p in g], axis=0)
            tokens = flat(own)
            n = norm(tokens, gain[1, 0:1], shift[1, 0:1])
            n2 = norm(flat(beside), gain[1, 0:1], shift[1, 0:1])
            q, k, v = project(n, wfull, 2)
            r2 = dot_rows(n2, wfull[1:3].reshape(2 * C, C))
            k2 = (r2[:, 0:128] + bqkv[2, 1:2]).astype(BF)
            v2 = (r2[:, 128:256] + bqkv[2, 2:3]).astype(BF)
            attended = []
            for first_window in range(0, span, PACK):
                group = [min(first_window + i, span - 1) for i in range(PACK)]
                queries, keys, values, key_ids = [], [], [], []
                for g in group:
                    at = slice(32 * g, 32 * g + 32)
                    queries.append(jnp.concatenate([q[at] * m for m in heads], axis=0))
                    keys.append(jnp.concatenate([k[at], k2[at]], axis=0))
                    values.append(jnp.concatenate([v[at], v2[at]], axis=0))
                    key_ids += own_id[g] + beside_id[g]
                key_id = jnp.concatenate(key_ids, axis=0).T[0:8]
                width = 64 * len(group)
                allowed = [
                    jnp.concatenate([i[:, 0:width] == key_id for i in own_id[g]] * 4, axis=0)
                    for g in group
                ]
                for parts in weighted(queries, keys, values, bias1.at[1 - is_bottom], allowed, 32)[: span - first_window]:
                    mixed = parts[3]
                    for h in (2, 1, 0):
                        mixed = jnp.where(head_of == h, parts[h], mixed)
                    attended.append(mixed.astype(BF))
            done = feed(1, jnp.concatenate(attended, axis=0), tokens)
            for g in range(span):
                for r in range(SHIFT):
                    i = 32 * g + 8 * r
                    y[mine + r, pl.ds(base + WIN * g, WIN), :] = done[i : i + 8]
            return carry

        lax.fori_loop(0, SPANS, body, 0)
        row = SHIFT * is_bottom
        for r in range(SHIFT):
            out_ref[row + r] = y[mine + r, SHIFT : SHIFT + cols, :].astype(BF)

    near = 1 - ch
    shifted_band(near)
    shifted_band(1 - near)

    for c in first + second + third + region_copies + side_copies:
        c.wait_send()
    for k in range(chunks):
        for near in (True, False):
            halo_copy(near, k).wait_send()
    for c in corner_copies(True) + corner_copies(False):
        c.wait_send()


def on_device(
    image_tokens, labels, rel_index, norm_gain, norm_shift, qkv_weight, qkv_bias, bias_table,
    proj_weight, proj_bias, fc1_weight, fc1_bias, fc2_weight, fc2_bias,
):
    rows, cols, _ = image_tokens.shape
    args = (
        image_tokens, labels, rel_index, norm_gain, norm_shift,
        jnp.swapaxes(qkv_weight, 2, 3), jnp.swapaxes(qkv_bias, 0, 1),
        jnp.swapaxes(bias_table, 1, 2),
        proj_weight, proj_bias, fc1_weight, fc1_bias, fc2_weight, fc2_bias,
    )
    V = pltpu.VMEM
    like = lambda a, *lead: V((*lead, *a.shape), a.dtype)
    copies = 34
    return pl.pallas_call(
        kernel,
        out_shape=pltpu.VMEM((rows, cols, C), BF),
        in_specs=[pl.BlockSpec(memory_space=pl.ANY)] * len(args),
        out_specs=pl.BlockSpec(memory_space=pltpu.VMEM),
        scratch_shapes=[
            like(image_tokens), like(labels), like(rel_index), like(norm_gain), like(norm_shift),
            like(args[6], 2), like(args[7], 2),
            V((2, C, C), BF), like(proj_bias),
            like(fc1_weight, 2), like(fc1_bias, 2), like(fc2_weight, 2), like(fc2_bias),
            V((3, C, C), BF), V((3, C, C), BF), V((3, C, C), BF),
            V((3, 3, C), F32),
            V((2, PACK, C, C), F32), V((2, PACK, C, C), F32),
            V((2 * WIN, cols + 8, C), F32), V((2 * WIN, cols + 8, C), F32),
            V((rows * cols, C), BF), V((rows * cols, C), BF),
            like(labels), like(labels, 8),
            V((rows, cols, C), BF), V((2, SHIFT, cols, C), BF),
            V((2, rows, 16, C), BF), V((4, SHIFT, 16, C), BF),
            pltpu.SemaphoreType.DMA((15,)),
            pltpu.SemaphoreType.DMA((copies,)),
            pltpu.SemaphoreType.DMA((copies,)),
        ],
        compiler_params=pltpu.CompilerParams(
            collective_id=0, has_side_effects=True, vmem_limit_bytes=60 * 1024 * 1024
        ),
        name="swin_pair",
    )(*args)


def solution(mesh):
    in_specs = (
        P(("row", "ch"), "col", None),
        P(("row", "ch"), "col"),
        P(),
        P(),
        P(),
        P(None, None, None, "ch"),
        P(None, None, "ch"),
        P(None, None, "ch"),
        P(None, "ch", None),
        P(),
        P(None, None, "ch"),
        P(None, "ch"),
        P(None, "ch", None),
        P(),
    )
    out_specs = P(("row", "ch"), "col", None)
    return jax.shard_map(
        on_device, mesh=mesh, in_specs=in_specs, out_specs=out_specs, check_vma=False
    )
```

```python
import functools
import math

import jax
import jax.numpy as jnp
from jax import lax
from jax.experimental import pallas as pl
from jax.experimental.pallas import tpu as pltpu
from jax.sharding import PartitionSpec as P

WIN = 8
SHIFT = 4
HEADS = 4
EPS = 1e-05
C = 128
HEAD = 32
BF = jnp.bfloat16
F32 = jnp.float32
LOG2E = math.log2(math.e)
QSCALE = LOG2E / math.sqrt(HEAD)
ROOT_HALF = math.sqrt(0.5)
EXCLUDED = -1e30
MESH = pl.DeviceIdType.MESH

GROUP = 8
CHUNK = GROUP * WIN
PACK = 2
SPANS = 3


def norm(x, gain, shift):
    center = x - jnp.mean(x, axis=-1, keepdims=True)
    spread = jnp.mean(center * center, axis=-1, keepdims=True)
    return (center * lax.rsqrt(spread + EPS) * gain + shift).astype(BF)


def dot(a, b):
    return jnp.dot(a, b, preferred_element_type=F32)


def dot_rows(a, b):
    return lax.dot_general(a, b, (((1,), (1,)), ((), ())), preferred_element_type=F32)


def kernel(
    x_in, lab_in, rel_in, gain_in, shift_in, qkvw_in, qkvb_in, tbl_in, projw_in,
    projb_in, fc1w_in, fc1b_in, fc2w_in, fc2b_in,
    out_ref,
    x, lab, rel, gain, shift, qkvb, tbl, wproj, projb, w1, b1, w2, fc2b,
    wown, woth, wfull, bqkv, bias0, bias1,
    y, ids, normed, att, region, lab_row, lab_side, lab_corner,
    halo, both, sides, corners,
    ready, local, send, recv,
):
    cols = x.shape[1]
    chunks = cols // CHUNK
    wins = cols // WIN + 1
    span = wins // SPANS
    groups = lax.axis_size("ch")
    bands = lax.axis_size("row") * groups
    tiles = lax.axis_size("col")
    ch = lax.axis_index("ch")
    col = lax.axis_index("col")
    band = lax.axis_index("row") * groups + ch

    def device(band_step, col_step):
        b = lax.rem(band + bands + band_step, bands)
        c = lax.rem(col + tiles + col_step, tiles)
        return {"row": b // groups, "col": c, "ch": lax.rem(b, groups)}

    partner = {"row": lax.axis_index("row"), "col": col, "ch": 1 - ch}
    across = {"row": lax.axis_index("row"), "col": lax.rem(col + tiles // 2, tiles), "ch": 1 - ch}
    up, down = device(-1, 0), device(1, 0)
    left, right = device(0, -1), device(0, 1)

    def towards(near):
        to_down = 1 - ch if near else ch
        return to_down, [device(2 * to_down - 1, side) for side in (0, -1, 1)]

    barrier = pltpu.get_barrier_semaphore()
    peers = [left, right, across] + towards(True)[1]
    strangers = towards(False)[1]

    def greet(semaphore, devices):
        for to in devices:
            pl.semaphore_signal(semaphore, inc=1, device_id=to, device_id_type=MESH)

    greet(barrier, peers)
    pl.when(ch == 0)(lambda: greet(barrier, strangers))

    def load(i, src, dst):
        return pltpu.make_async_copy(src, dst, local.at[i])

    own_rows = pl.ds(0, 64)
    other_rows = pl.ds(64, 64)
    early = [
        load(0, x_in, x),
        load(1, qkvw_in.at[0], wown.at[:, own_rows]),
        load(2, qkvb_in, qkvb.at[0]),
        load(3, tbl_in, tbl.at[0]),
        load(4, rel_in, rel),
        load(5, gain_in, gain),
        load(6, shift_in, shift),
    ]
    late = [
        load(7, projw_in, wproj.at[:, own_rows]),
        load(8, fc1w_in, w1.at[0]),
        load(9, fc1b_in, b1.at[0]),
        load(10, fc2w_in, w2.at[0]),
        load(11, qkvw_in.at[1], wfull.at[:, own_rows]),
        load(12, projb_in, projb),
        load(13, fc2b_in, fc2b),
        load(14, lab_in, lab),
    ]
    for c in early + late:
        c.start()

    wown[:, 64:128, :] = jnp.zeros((3, 64, C), BF)
    woth[:, 0:64, :] = jnp.zeros((3, 64, C), BF)

    def copy(i, src, dst, to):
        return pltpu.make_async_remote_copy(
            src_ref=src, dst_ref=dst, send_sem=send.at[i], recv_sem=recv.at[i],
            device_id=to, device_id_type=MESH,
        )

    first = [
        copy(0, wown.at[:, own_rows], woth.at[:, other_rows], partner),
        copy(1, qkvb.at[0], qkvb.at[1], partner),
        copy(2, tbl.at[0], tbl.at[1], partner),
        copy(3, b1.at[0], b1.at[1], partner),
    ]
    def feed_copies(b):
        return [
            copy(4 + 4 * b, wproj.at[b, own_rows], wproj.at[b, other_rows], across),
            copy(5 + 4 * b, w1.at[0, b], w1.at[1, b], (partner, across)[b]),
            copy(6 + 4 * b, w2.at[0, b], w2.at[1, b], across),
        ]
    second = feed_copies(0)
    third = [copy(7, wfull.at[:, own_rows], wfull.at[:, other_rows], across)] + feed_copies(1)
    half_at = {-1: pl.ds(0, 128), 1: pl.ds(cols - 128, 128)}
    side_regions = [
        copy(13, region.at[:, :, half_at[-1]], lab_side.at[1], left),
        copy(14, region.at[:, :, half_at[1]], lab_side.at[0], right),
    ]

    def band_regions(near):
        to_down, (to, *diagonals) = towards(near)
        return [copy(11 + to_down, region.at[to_down], lab_row.at[to_down], to)] + [
            copy(
                15 + 2 * to_down + i, region.at[to_down, :, half_at[side]],
                lab_corner.at[2 * to_down + i], diagonals[i],
            )
            for i, side in enumerate((-1, 1))
        ]

    for c in early:
        c.wait()

    lane = lax.broadcasted_iota(jnp.int32, (1, C), 1)
    head_of = lane // HEAD
    heads = [(head_of == h).astype(F32).astype(BF) for h in range(HEADS)]

    entries = tbl.shape[-1]

    def lookup(index, side, b, h):
        line = tbl[side, b, h : h + 1, :]
        a0 = jnp.broadcast_to(line[:, 0:128], index.shape)
        a1 = jnp.concatenate([line[:, 128:], jnp.zeros((1, 256 - entries), F32)], axis=1)
        a1 = jnp.broadcast_to(a1, index.shape)
        within = jnp.bitwise_and(index, 127)
        g0 = jnp.take_along_axis(a0, within, axis=1)
        g1 = jnp.take_along_axis(a1, within, axis=1)
        return jnp.where(index < 128, g0, g1) * LOG2E

    def put_bias(bias, i, rows, values):
        bias[i, 0, rows] = jnp.where(lane < 64, values, EXCLUDED)
        bias[i, 1, rows] = jnp.where(lane < 64, EXCLUDED, values)

    def first_bias(side):
        twice = jnp.concatenate([rel[...], rel[...]], axis=1)
        for h in range(2):
            put_bias(bias0, side, slice(64 * h, 64 * h + 64), lookup(twice, side, 0, h))

    def zero_padded(values, side):
        pad = jnp.zeros_like(values)
        return jnp.concatenate([values, pad] if side == 0 else [pad, values], axis=1)

    first_bias(0)
    for m in range(3):
        bqkv[0, m : m + 1] = zero_padded(qkvb[0, m, 0:1], 0)

    def project(n, w, b):
        r = dot_rows(n, w[...].reshape(3 * C, C))
        q = ((r[:, 0:128] + bqkv[b, 0:1]) * QSCALE).astype(BF)
        k = (r[:, 128:256] + bqkv[b, 1:2]).astype(BF)
        v = (r[:, 256:384] + bqkv[b, 2:3]).astype(BF)
        return q, k, v

    def weighted(queries, keys, values, bias, allowed, each):
        width = 64 * len(queries)
        s = dot_rows(jnp.concatenate(queries, axis=0), jnp.concatenate(keys, axis=0))
        s = [s[C * i : C * i + C] + bias[i, :, 0:width] for i in range(len(queries))]
        if allowed is not None:
            s = [jnp.where(a, b, EXCLUDED) for a, b in zip(allowed, s)]
        raised = [jnp.exp2(a - jnp.max(a, axis=1, keepdims=True)) for a in s]
        totals = [jnp.sum(a, axis=1, keepdims=True) for a in raised]
        o = dot(
            jnp.concatenate([a.astype(BF) for a in raised], axis=0),
            jnp.concatenate(values, axis=0),
        )
        mixed = []
        for i, total in enumerate(totals):
            part = o[C * i : C * i + C] * (1.0 / total)
            mixed.append([part[k : k + each] for k in range(0, C, each)])
        return mixed

    def half_attention(side, q, k, v):
        cut = lambda a: [a[64 * g : 64 * g + 64] for g in range(GROUP)]
        stacked = [
            jnp.concatenate([a * heads[2 * side], a * heads[2 * side + 1]], axis=0) for a in cut(q)
        ]
        k, v = cut(k), cut(v)
        out = []
        for g in range(0, GROUP, 2):
            two = slice(g, g + 2)
            for o0, o1 in weighted(stacked[two], k[two], v[two], bias0.at[side], None, 64):
                out.append(jnp.where(head_of == 2 * side, o0, o1).astype(BF))
        return jnp.concatenate(out, axis=0)

    def windows_of(base):
        lines = [x[r, pl.ds(base, CHUNK), :].astype(F32) for r in range(WIN)]
        return jnp.concatenate(
            [lines[r][WIN * g : WIN * g + WIN] for g in range(GROUP) for r in range(WIN)], axis=0
        )

    def meet():
        for c in late:
            c.wait()
        i = lax.broadcasted_iota(jnp.int32, lab.shape, 0)
        j = lax.broadcasted_iota(jnp.int32, lab.shape, 1)
        first_band = (band == 0).astype(jnp.int32)
        first_tile = (col == 0).astype(jnp.int32)
        regions = (
            lab[...] * 4
            + (i < SHIFT).astype(jnp.int32) * (2 * first_band)
            + (j < SHIFT).astype(jnp.int32) * first_tile
        )
        for half in range(2):
            region[half] = regions[SHIFT * half : SHIFT * half + SHIFT]

        pl.semaphore_wait(barrier, len(peers) + len(strangers) * ch)
        pl.when(ch == 1)(lambda: greet(ready, strangers))
        for c in first + second + third + side_regions + band_regions(True):
            c.start()

    def own_heads(j, carry):
        pl.when(j == 1)(meet)
        base = pl.multiple_of(j * CHUNK, CHUNK)
        at = pl.ds(pl.multiple_of(j * 64 * GROUP, 64 * GROUP), 64 * GROUP)
        n = norm(windows_of(base), gain[0, 0:1], shift[0, 0:1])
        normed[at, :] = n
        q, k, v = project(n, wown, 0)
        att[at, :] = half_attention(0, q, k, v)
        return carry

    lax.fori_loop(0, chunks, own_heads, 0)

    for c in first:
        c.wait_recv()
    first_bias(1)
    for m in range(3):
        bqkv[1, m : m + 1] = zero_padded(qkvb[1, m, 0:1], 1)
        bqkv[2, m : m + 1] = jnp.concatenate([qkvb[0, m, 1:2], qkvb[1, m, 1:2]], axis=1)
    for t, part in enumerate(
        (rel[0:32], jnp.concatenate([rel[32:64, 32:64], rel[32:64, 0:32]], axis=1))
    ):
        index = jnp.concatenate([part, part], axis=1)
        for h in range(HEADS):
            put_bias(bias1, t, slice(32 * h, 32 * h + 32), lookup(index, h // 2, 1, h % 2))

    def feed(b, attended, tokens):
        mid = (tokens + dot(attended, wproj[b]) + projb[b : b + 1]).astype(BF).astype(F32)
        n = norm(mid, gain[b, 1:2], shift[b, 1:2])
        total = mid + fc2b[b : b + 1]
        for side in range(2):
            inner = dot(n, w1[side, b]) + b1[side, b : b + 1]
            hidden = (inner * (0.5 + 0.5 * lax.erf(inner * ROOT_HALF))).astype(BF)
            total = total + dot(hidden, w2[side, b])
        return total.astype(BF).astype(F32)

    for c in second:
        c.wait_recv()

    def halo_copy(near, k):
        at = pl.ds(pl.multiple_of(k * CHUNK, CHUNK), CHUNK)
        to_down = towards(near)[0]
        return copy(
            20 + 4 * to_down + k, halo.at[pl.ds(SHIFT * to_down, SHIFT), at],
            both.at[to_down, :, at], towards(near)[1][0],
        )

    edge = {-1: pl.ds(0, 16), 1: pl.ds(cols - 16, 16)}
    side_copies = [
        copy(28, halo.at[:, edge[-1]], sides.at[1], left),
        copy(29, halo.at[:, edge[1]], sides.at[0], right),
    ]

    def corner_copies(near):
        to_down, (_, *diagonals) = towards(near)
        return [
            copy(
                30 + 2 * to_down + i, halo.at[pl.ds(SHIFT * to_down, SHIFT), edge[side]],
                corners.at[2 * to_down + i], diagonals[i],
            )
            for i, side in enumerate((-1, 1))
        ]

    def first_block(step, carry):
        k = lax.rem(step + chunks - 1, chunks)
        base = pl.multiple_of(k * CHUNK, CHUNK)
        at = pl.ds(pl.multiple_of(k * 64 * GROUP, 64 * GROUP), 64 * GROUP)
        q, key, v = project(normed[at, :], woth, 1)
        other = half_attention(1, q, key, v)
        done = feed(0, att[at, :] + other, windows_of(base))
        for r in range(WIN):
            line = jnp.concatenate(
                [done[64 * g + 8 * r : 64 * g + 8 * r + 8] for g in range(GROUP)], axis=0
            )
            y[SHIFT + r, pl.ds(base + SHIFT, CHUNK), :] = line
            halo[r, pl.ds(base, CHUNK), :] = line.astype(BF)
        halo_copy(True, k).start()

        @pl.when(step == 1)
        def _():
            for c in side_copies + corner_copies(True):
                c.start()

        return carry

    lax.fori_loop(0, chunks, first_block, 0)

    pl.when(ch == 0)(lambda: pl.semaphore_wait(ready, len(strangers)))
    for c in band_regions(False):
        c.start()
    for k in range(chunks):
        halo_copy(False, k).start()
    for c in corner_copies(False):
        c.start()

    def spread(line):
        return jnp.broadcast_to(line.astype(F32), (128, 128)).T

    def put_ids(row, middle, before, after):
        for r in range(SHIFT):
            line = slice(r, r + 1)
            for t in range(cols // 128):
                ids[row + r, SHIFT + 128 * t : SHIFT + 128 * t + 128, :] = spread(
                    middle[line, 128 * t : 128 * t + 128]
                )
            ids[row + r, 0:SHIFT, :] = spread(before[line])[128 - SHIFT :]
            ids[row + r, SHIFT + cols : 2 * SHIFT + cols, :] = spread(after[line])[0:SHIFT]

    for c in side_regions:
        c.wait_recv()
    for half in range(2):
        put_ids(
            SHIFT + SHIFT * half, region.at[half], lab_side.at[0, half], lab_side.at[1, half]
        )

    for c in third:
        c.wait_recv()
    for c in side_copies:
        c.wait_recv()
    ends = ((slice(0, SHIFT), slice(12, 16)), (slice(SHIFT + cols, 2 * SHIFT + cols), slice(0, SHIFT)))
    for s, (to, of) in enumerate(ends):
        for r in range(WIN):
            y[SHIFT + r, to, :] = sides[s, r].astype(F32)[of]

    def shifted_band(is_bottom):
        mine = SHIFT + SHIFT * is_bottom
        theirs = (SHIFT + WIN) * is_bottom

        arrived = both.at[1 - is_bottom]
        flow = 20 + 4 * (1 - is_bottom)

        def take(k):
            at = pl.ds(pl.multiple_of(k * CHUNK, CHUNK), CHUNK)
            copy(flow + k, arrived.at[:, at], arrived.at[:, at], up).wait_recv()
            for r in range(SHIFT):
                y[theirs + r, pl.ds(k * CHUNK + SHIFT, CHUNK), :] = arrived[r, at, :].astype(F32)

        above = 1 - is_bottom
        corner = 2 * above
        copy(11 + above, lab_row.at[above], lab_row.at[above], up).wait_recv()
        for i in range(2):
            part = lab_corner.at[corner + i]
            copy(15 + corner + i, part, part, up).wait_recv()
        put_ids(theirs, lab_row.at[above], lab_corner.at[corner + 1], lab_corner.at[corner])
        for i in range(2):
            part = corners.at[corner + i]
            copy(30 + corner + i, part, part, up).wait_recv()
            to, of = ends[1 - i]
            for r in range(SHIFT):
                y[theirs + r, to, :] = part[r].astype(F32)[of]
        take(0)

        def body(c, carry):
            take(c + 1)
            base = pl.multiple_of(c * span * WIN, WIN)

            def gather(ref, row):
                return [
                    [ref[row + r, pl.ds(base + WIN * g, WIN), :] for r in range(SHIFT)]
                    for g in range(span)
                ]

            own = gather(y, mine)
            beside = gather(y, theirs)
            own_id = gather(ids, mine)
            beside_id = gather(ids, theirs)
            flat = lambda parts: jnp.concatenate([p for g in parts for p in g], axis=0)
            tokens = flat(own)
            n = norm(tokens, gain[1, 0:1], shift[1, 0:1])
            n2 = norm(flat(beside), gain[1, 0:1], shift[1, 0:1])
            q, k, v = project(n, wfull, 2)
            r2 = dot_rows(n2, wfull[1:3].reshape(2 * C, C))
            k2 = (r2[:, 0:128] + bqkv[2, 1:2]).astype(BF)
            v2 = (r2[:, 128:256] + bqkv[2, 2:3]).astype(BF)
            attended = []
            for first_window in range(0, span, PACK):
                group = [min(first_window + i, span - 1) for i in range(PACK)]
                queries, keys, values, key_ids = [], [], [], []
                for g in group:
                    at = slice(32 * g, 32 * g + 32)
                    queries.append(jnp.concatenate([q[at] * m for m in heads], axis=0))
                    keys.append(jnp.concatenate([k[at], k2[at]], axis=0))
                    values.append(jnp.concatenate([v[at], v2[at]], axis=0))
                    key_ids += own_id[g] + beside_id[g]
                key_id = jnp.concatenate(key_ids, axis=0).T[0:8]
                width = 64 * len(group)
                allowed = [
                    jnp.concatenate([i[:, 0:width] == key_id for i in own_id[g]] * 4, axis=0)
                    for g in group
                ]
                for parts in weighted(queries, keys, values, bias1.at[1 - is_bottom], allowed, 32)[: span - first_window]:
                    mixed = parts[3]
                    for h in (2, 1, 0):
                        mixed = jnp.where(head_of == h, parts[h], mixed)
                    attended.append(mixed.astype(BF))
            done = feed(1, jnp.concatenate(attended, axis=0), tokens)
            for g in range(span):
                for r in range(SHIFT):
                    i = 32 * g + 8 * r
                    y[mine + r, pl.ds(base + WIN * g, WIN), :] = done[i : i + 8]
            return carry

        lax.fori_loop(0, SPANS, body, 0)
        row = SHIFT * is_bottom
        for r in range(SHIFT):
            out_ref[row + r] = y[mine + r, SHIFT : SHIFT + cols, :].astype(BF)

    shifted_band(1 - ch)
    shifted_band(ch)

    for c in first + second + third + side_regions + side_copies:
        c.wait_send()
    for k in range(chunks):
        for near in (True, False):
            halo_copy(near, k).wait_send()
    for near in (True, False):
        for c in corner_copies(near) + band_regions(near):
            c.wait_send()


def on_device(
    image_tokens, labels, rel_index, norm_gain, norm_shift, qkv_weight, qkv_bias, bias_table,
    proj_weight, proj_bias, fc1_weight, fc1_bias, fc2_weight, fc2_bias,
):
    rows, cols, _ = image_tokens.shape
    args = (
        image_tokens, labels, rel_index, norm_gain, norm_shift,
        jnp.swapaxes(qkv_weight, 2, 3), jnp.swapaxes(qkv_bias, 0, 1),
        jnp.swapaxes(bias_table, 1, 2),
        proj_weight, proj_bias, fc1_weight, fc1_bias, fc2_weight, fc2_bias,
    )
    V = pltpu.VMEM
    like = lambda a, *lead: V((*lead, *a.shape), a.dtype)
    copies = 34
    return pl.pallas_call(
        kernel,
        out_shape=pltpu.VMEM((rows, cols, C), BF),
        in_specs=[pl.BlockSpec(memory_space=pl.ANY)] * len(args),
        out_specs=pl.BlockSpec(memory_space=pltpu.VMEM),
        scratch_shapes=[
            like(image_tokens), like(labels), like(rel_index), like(norm_gain), like(norm_shift),
            like(args[6], 2), like(args[7], 2),
            V((2, C, C), BF), like(proj_bias),
            like(fc1_weight, 2), like(fc1_bias, 2), like(fc2_weight, 2), like(fc2_bias),
            V((3, C, C), BF), V((3, C, C), BF), V((3, C, C), BF),
            V((3, 3, C), F32),
            V((2, PACK, C, C), F32), V((2, PACK, C, C), F32),
            V((2 * WIN, cols + 8, C), F32), V((2 * WIN, cols + 8, C), F32),
            V((rows * cols, C), BF), V((rows * cols, C), BF),
            V((2, SHIFT, cols), jnp.int32), V((2, SHIFT, cols), jnp.int32),
            V((2, 2, SHIFT, 128), jnp.int32), V((4, SHIFT, 128), jnp.int32),
            V((rows, cols, C), BF), V((2, SHIFT, cols, C), BF),
            V((2, rows, 16, C), BF), V((4, SHIFT, 16, C), BF),
            pltpu.SemaphoreType.REGULAR,
            pltpu.SemaphoreType.DMA((15,)),
            pltpu.SemaphoreType.DMA((copies,)),
            pltpu.SemaphoreType.DMA((copies,)),
        ],
        compiler_params=pltpu.CompilerParams(
            collective_id=0, has_side_effects=True, vmem_limit_bytes=60 * 1024 * 1024
        ),
        name="swin_pair",
    )(*args)


def solution(mesh):
    in_specs = (
        P(("row", "ch"), "col", None),
        P(("row", "ch"), "col"),
        P(),
        P(),
        P(),
        P(None, None, None, "ch"),
        P(None, None, "ch"),
        P(None, None, "ch"),
        P(None, "ch", None),
        P(),
        P(None, None, "ch"),
        P(None, "ch"),
        P(None, "ch", None),
        P(),
    )
    out_specs = P(("row", "ch"), "col", None)
    return jax.shard_map(
        on_device, mesh=mesh, in_specs=in_specs, out_specs=out_specs, check_vma=False
    )
```

```python
import functools
import math

import jax
import jax.numpy as jnp
from jax import lax
from jax.experimental import pallas as pl
from jax.experimental.pallas import tpu as pltpu
from jax.sharding import PartitionSpec as P

WIN = 8
SHIFT = 4
HEADS = 4
EPS = 1e-05
C = 128
HEAD = 32
BF = jnp.bfloat16
F32 = jnp.float32
LOG2E = math.log2(math.e)
QSCALE = LOG2E / math.sqrt(HEAD)
ROOT_HALF = math.sqrt(0.5)
EXCLUDED = -1e30
MESH = pl.DeviceIdType.MESH

GROUP = 8
CHUNK = GROUP * WIN
PACK = 2
SPANS = 3


def norm(x, gain, shift):
    center = x - jnp.mean(x, axis=-1, keepdims=True)
    spread = jnp.mean(center * center, axis=-1, keepdims=True)
    return (center * lax.rsqrt(spread + EPS) * gain + shift).astype(BF)


def dot(a, b):
    return jnp.dot(a, b, preferred_element_type=F32)


def dot_rows(a, b):
    return lax.dot_general(a, b, (((1,), (1,)), ((), ())), preferred_element_type=F32)


def kernel(
    x_in, lab_in, rel_in, gain_in, shift_in, qkvw_in, qkvb_in, tbl_in, projw_in,
    projb_in, fc1w_in, fc1b_in, fc2w_in, fc2b_in,
    out_ref,
    x, lab, rel, gain, shift, qkvb, tbl, wproj, projb, w1, b1, w2, fc2b,
    wown, woth, wfull, bqkv, bias0, bias1,
    y, ids, normed, att, region, lab_row, lab_side, lab_corner,
    halo, both, sides, corners,
    ready, local, send, recv,
):
    cols = x.shape[1]
    chunks = cols // CHUNK
    wins = cols // WIN + 1
    span = wins // SPANS
    groups = lax.axis_size("ch")
    bands = lax.axis_size("row") * groups
    tiles = lax.axis_size("col")
    ch = lax.axis_index("ch")
    col = lax.axis_index("col")
    band = lax.axis_index("row") * groups + ch

    def device(band_step, col_step):
        b = lax.rem(band + bands + band_step, bands)
        c = lax.rem(col + tiles + col_step, tiles)
        return {"row": b // groups, "col": c, "ch": lax.rem(b, groups)}

    partner = {"row": lax.axis_index("row"), "col": col, "ch": 1 - ch}
    across = {"row": lax.axis_index("row"), "col": lax.rem(col + tiles // 2, tiles), "ch": 1 - ch}
    up, down = device(-1, 0), device(1, 0)
    left, right = device(0, -1), device(0, 1)

    def towards(near):
        to_down = 1 - ch if near else ch
        return to_down, [device(2 * to_down - 1, side) for side in (0, -1, 1)]

    barrier = pltpu.get_barrier_semaphore()
    peers = [left, right, across] + towards(True)[1]
    strangers = towards(False)[1]

    def greet(semaphore, devices):
        for to in devices:
            pl.semaphore_signal(semaphore, inc=1, device_id=to, device_id_type=MESH)

    greet(barrier, peers)
    pl.when(ch == 0)(lambda: greet(barrier, strangers))

    def load(i, src, dst):
        return pltpu.make_async_copy(src, dst, local.at[i])

    own_rows = pl.ds(0, 64)
    other_rows = pl.ds(64, 64)
    early = [
        load(0, x_in, x),
        load(1, qkvw_in.at[0], wown.at[:, own_rows]),
        load(2, qkvb_in, qkvb.at[0]),
        load(3, tbl_in, tbl.at[0]),
        load(4, rel_in, rel),
        load(5, gain_in, gain),
        load(6, shift_in, shift),
    ]
    late = [
        load(7, projw_in, wproj.at[:, own_rows]),
        load(8, fc1w_in, w1.at[0]),
        load(9, fc1b_in, b1.at[0]),
        load(10, fc2w_in, w2.at[0]),
        load(11, qkvw_in.at[1], wfull.at[:, own_rows]),
        load(12, projb_in, projb),
        load(13, fc2b_in, fc2b),
        load(14, lab_in, lab),
    ]
    for c in early + late:
        c.start()

    wown[:, 64:128, :] = jnp.zeros((3, 64, C), BF)
    woth[:, 0:64, :] = jnp.zeros((3, 64, C), BF)

    def copy(i, src, dst, to):
        return pltpu.make_async_remote_copy(
            src_ref=src, dst_ref=dst, send_sem=send.at[i], recv_sem=recv.at[i],
            device_id=to, device_id_type=MESH,
        )

    first = [
        copy(0, wown.at[:, own_rows], woth.at[:, other_rows], partner),
        copy(1, qkvb.at[0], qkvb.at[1], partner),
        copy(2, tbl.at[0], tbl.at[1], partner),
        copy(3, b1.at[0], b1.at[1], partner),
    ]
    def feed_copies(b):
        return [
            copy(4 + 4 * b, wproj.at[b, own_rows], wproj.at[b, other_rows], across),
            copy(5 + 4 * b, w1.at[0, b], w1.at[1, b], (partner, across)[b]),
            copy(6 + 4 * b, w2.at[0, b], w2.at[1, b], across),
        ]
    second = feed_copies(0)
    third = [copy(7, wfull.at[:, own_rows], wfull.at[:, other_rows], across)] + feed_copies(1)
    half_at = {-1: pl.ds(0, 128), 1: pl.ds(cols - 128, 128)}
    side_regions = [
        copy(13, region.at[:, :, half_at[-1]], lab_side.at[1], left),
        copy(14, region.at[:, :, half_at[1]], lab_side.at[0], right),
    ]

    def band_regions(near):
        to_down, (to, *diagonals) = towards(near)
        return [copy(11 + to_down, region.at[to_down], lab_row.at[to_down], to)] + [
            copy(
                15 + 2 * to_down + i, region.at[to_down, :, half_at[side]],
                lab_corner.at[2 * to_down + i], diagonals[i],
            )
            for i, side in enumerate((-1, 1))
        ]

    for c in early:
        c.wait()

    lane = lax.broadcasted_iota(jnp.int32, (1, C), 1)
    head_of = lane // HEAD
    heads = [(head_of == h).astype(F32).astype(BF) for h in range(HEADS)]

    entries = tbl.shape[-1]

    def lookup(index, side, b, h):
        line = tbl[side, b, h : h + 1, :]
        a0 = jnp.broadcast_to(line[:, 0:128], index.shape)
        a1 = jnp.concatenate([line[:, 128:], jnp.zeros((1, 256 - entries), F32)], axis=1)
        a1 = jnp.broadcast_to(a1, index.shape)
        within = jnp.bitwise_and(index, 127)
        g0 = jnp.take_along_axis(a0, within, axis=1)
        g1 = jnp.take_along_axis(a1, within, axis=1)
        return jnp.where(index < 128, g0, g1) * LOG2E

    def put_bias(bias, i, rows, values):
        bias[i, 0, rows] = jnp.where(lane < 64, values, EXCLUDED)
        bias[i, 1, rows] = jnp.where(lane < 64, EXCLUDED, values)

    def first_bias(side):
        twice = jnp.concatenate([rel[...], rel[...]], axis=1)
        for h in range(2):
            put_bias(bias0, side, slice(64 * h, 64 * h + 64), lookup(twice, side, 0, h))

    def zero_padded(values, side):
        pad = jnp.zeros_like(values)
        return jnp.concatenate([values, pad] if side == 0 else [pad, values], axis=1)

    first_bias(0)
    for m in range(3):
        bqkv[0, m : m + 1] = zero_padded(qkvb[0, m, 0:1], 0)

    def project(n, w, b):
        r = dot_rows(n, w[...].reshape(3 * C, C))
        q = ((r[:, 0:128] + bqkv[b, 0:1]) * QSCALE).astype(BF)
        k = (r[:, 128:256] + bqkv[b, 1:2]).astype(BF)
        v = (r[:, 256:384] + bqkv[b, 2:3]).astype(BF)
        return q, k, v

    def weighted(queries, keys, values, bias, allowed, each):
        width = 64 * len(queries)
        s = dot_rows(jnp.concatenate(queries, axis=0), jnp.concatenate(keys, axis=0))
        s = [s[C * i : C * i + C] + bias[i, :, 0:width] for i in range(len(queries))]
        if allowed is not None:
            s = [jnp.where(a, b, EXCLUDED) for a, b in zip(allowed, s)]
        raised = [jnp.exp2(a - jnp.max(a, axis=1, keepdims=True)) for a in s]
        totals = [jnp.sum(a, axis=1, keepdims=True) for a in raised]
        o = dot(
            jnp.concatenate([a.astype(BF) for a in raised], axis=0),
            jnp.concatenate(values, axis=0),
        )
        mixed = []
        for i, total in enumerate(totals):
            part = o[C * i : C * i + C] * (1.0 / total)
            mixed.append([part[k : k + each] for k in range(0, C, each)])
        return mixed

    def half_attention(side, q, k, v):
        cut = lambda a: [a[64 * g : 64 * g + 64] for g in range(GROUP)]
        stacked = [
            jnp.concatenate([a * heads[2 * side], a * heads[2 * side + 1]], axis=0) for a in cut(q)
        ]
        k, v = cut(k), cut(v)
        out = []
        for g in range(0, GROUP, 2):
            two = slice(g, g + 2)
            for o0, o1 in weighted(stacked[two], k[two], v[two], bias0.at[side], None, 64):
                out.append(jnp.where(head_of == 2 * side, o0, o1).astype(BF))
        return jnp.concatenate(out, axis=0)

    def windows_of(base):
        lines = [x[r, pl.ds(base, CHUNK), :].astype(F32) for r in range(WIN)]
        return jnp.concatenate(
            [lines[r][WIN * g : WIN * g + WIN] for g in range(GROUP) for r in range(WIN)], axis=0
        )

    def meet():
        for c in late:
            c.wait()
        i = lax.broadcasted_iota(jnp.int32, lab.shape, 0)
        j = lax.broadcasted_iota(jnp.int32, lab.shape, 1)
        first_band = (band == 0).astype(jnp.int32)
        first_tile = (col == 0).astype(jnp.int32)
        regions = (
            lab[...] * 4
            + (i < SHIFT).astype(jnp.int32) * (2 * first_band)
            + (j < SHIFT).astype(jnp.int32) * first_tile
        )
        for half in range(2):
            region[half] = regions[SHIFT * half : SHIFT * half + SHIFT]

        pl.semaphore_wait(barrier, len(peers) + len(strangers) * ch)
        pl.when(ch == 1)(lambda: greet(ready, strangers))
        for c in first + second + third + side_regions + band_regions(True):
            c.start()

    def own_heads(j, carry):
        pl.when(j == 1)(meet)
        base = pl.multiple_of(j * CHUNK, CHUNK)
        at = pl.ds(pl.multiple_of(j * 64 * GROUP, 64 * GROUP), 64 * GROUP)
        n = norm(windows_of(base), gain[0, 0:1], shift[0, 0:1])
        normed[at, :] = n
        q, k, v = project(n, wown, 0)
        att[at, :] = half_attention(0, q, k, v)
        return carry

    lax.fori_loop(0, chunks, own_heads, 0)

    def spread(line):
        return jnp.broadcast_to(line.astype(F32), (128, 128)).T

    def put_middle(row, middle):
        for r in range(SHIFT):
            for t in range(cols // 128):
                ids[row + r, SHIFT + 128 * t : SHIFT + 128 * t + 128, :] = spread(
                    middle[r : r + 1, 128 * t : 128 * t + 128]
                )

    def put_ends(row, before, after):
        for r in range(SHIFT):
            line = slice(r, r + 1)
            ids[row + r, 0:SHIFT, :] = spread(before[line])[128 - SHIFT :]
            ids[row + r, SHIFT + cols : 2 * SHIFT + cols, :] = spread(after[line])[0:SHIFT]

    for half in range(2):
        put_middle(SHIFT + SHIFT * half, region.at[half])

    for c in first:
        c.wait_recv()
    first_bias(1)
    for m in range(3):
        bqkv[1, m : m + 1] = zero_padded(qkvb[1, m, 0:1], 1)
        bqkv[2, m : m + 1] = jnp.concatenate([qkvb[0, m, 1:2], qkvb[1, m, 1:2]], axis=1)
    for t, part in enumerate(
        (rel[0:32], jnp.concatenate([rel[32:64, 32:64], rel[32:64, 0:32]], axis=1))
    ):
        index = jnp.concatenate([part, part], axis=1)
        for h in range(HEADS):
            put_bias(bias1, t, slice(32 * h, 32 * h + 32), lookup(index, h // 2, 1, h % 2))

    def feed(b, attended, tokens):
        mid = (tokens + dot(attended, wproj[b]) + projb[b : b + 1]).astype(BF).astype(F32)
        n = norm(mid, gain[b, 1:2], shift[b, 1:2])
        total = mid + fc2b[b : b + 1]
        for side in range(2):
            inner = dot(n, w1[side, b]) + b1[side, b : b + 1]
            hidden = (inner * (0.5 + 0.5 * lax.erf(inner * ROOT_HALF))).astype(BF)
            total = total + dot(hidden, w2[side, b])
        return total.astype(BF).astype(F32)

    def halo_copy(near, k):
        at = pl.ds(pl.multiple_of(k * CHUNK, CHUNK), CHUNK)
        to_down = towards(near)[0]
        return copy(
            20 + 4 * to_down + k, halo.at[pl.ds(SHIFT * to_down, SHIFT), at],
            both.at[to_down, :, at], towards(near)[1][0],
        )

    edge = {-1: pl.ds(0, 16), 1: pl.ds(cols - 16, 16)}
    side_copies = [
        copy(28, halo.at[:, edge[-1]], sides.at[1], left),
        copy(29, halo.at[:, edge[1]], sides.at[0], right),
    ]

    def corner_copies(near):
        to_down, (_, *diagonals) = towards(near)
        return [
            copy(
                30 + 2 * to_down + i, halo.at[pl.ds(SHIFT * to_down, SHIFT), edge[side]],
                corners.at[2 * to_down + i], diagonals[i],
            )
            for i, side in enumerate((-1, 1))
        ]

    def first_block(step, carry):
        k = lax.rem(step + chunks - 1, chunks)
        base = pl.multiple_of(k * CHUNK, CHUNK)
        at = pl.ds(pl.multiple_of(k * 64 * GROUP, 64 * GROUP), 64 * GROUP)
        q, key, v = project(normed[at, :], woth, 1)
        other = half_attention(1, q, key, v)

        @pl.when(step == 0)
        def _():
            for c in second:
                c.wait_recv()

        done = feed(0, att[at, :] + other, windows_of(base))
        for r in range(WIN):
            line = jnp.concatenate(
                [done[64 * g + 8 * r : 64 * g + 8 * r + 8] for g in range(GROUP)], axis=0
            )
            y[SHIFT + r, pl.ds(base + SHIFT, CHUNK), :] = line
            halo[r, pl.ds(base, CHUNK), :] = line.astype(BF)
        halo_copy(True, k).start()

        @pl.when(step == 1)
        def _():
            for c in side_copies + corner_copies(True):
                c.start()

        return carry

    lax.fori_loop(0, chunks, first_block, 0)

    pl.when(ch == 0)(lambda: pl.semaphore_wait(ready, len(strangers)))
    for c in band_regions(False) + corner_copies(False):
        c.start()
    for k in range(chunks):
        halo_copy(False, k).start()

    for c in side_regions:
        c.wait_recv()
    for half in range(2):
        put_ends(SHIFT + SHIFT * half, lab_side.at[0, half], lab_side.at[1, half])

    for c in third:
        c.wait_recv()
    for c in side_copies:
        c.wait_recv()
    ends = ((slice(0, SHIFT), slice(12, 16)), (slice(SHIFT + cols, 2 * SHIFT + cols), slice(0, SHIFT)))
    for s, (to, of) in enumerate(ends):
        for r in range(WIN):
            y[SHIFT + r, to, :] = sides[s, r].astype(F32)[of]

    def shifted_band(is_bottom):
        mine = SHIFT + SHIFT * is_bottom
        theirs = (SHIFT + WIN) * is_bottom

        arrived = both.at[1 - is_bottom]
        flow = 20 + 4 * (1 - is_bottom)

        def take(k):
            at = pl.ds(pl.multiple_of(k * CHUNK, CHUNK), CHUNK)
            copy(flow + k, arrived.at[:, at], arrived.at[:, at], up).wait_recv()
            for r in range(SHIFT):
                y[theirs + r, pl.ds(k * CHUNK + SHIFT, CHUNK), :] = arrived[r, at, :].astype(F32)

        above = 1 - is_bottom
        corner = 2 * above
        copy(11 + above, lab_row.at[above], lab_row.at[above], up).wait_recv()
        for i in range(2):
            part = lab_corner.at[corner + i]
            copy(15 + corner + i, part, part, up).wait_recv()
        put_middle(theirs, lab_row.at[above])
        put_ends(theirs, lab_corner.at[corner + 1], lab_corner.at[corner])
        for i in range(2):
            part = corners.at[corner + i]
            copy(30 + corner + i, part, part, up).wait_recv()
            to, of = ends[1 - i]
            for r in range(SHIFT):
                y[theirs + r, to, :] = part[r].astype(F32)[of]
        take(0)

        def body(c, carry):
            take(c + 1)
            base = pl.multiple_of(c * span * WIN, WIN)

            def gather(ref, row):
                return [
                    [ref[row + r, pl.ds(base + WIN * g, WIN), :] for r in range(SHIFT)]
                    for g in range(span)
                ]

            own = gather(y, mine)
            beside = gather(y, theirs)
            own_id = gather(ids, mine)
            beside_id = gather(ids, theirs)
            flat = lambda parts: jnp.concatenate([p for g in parts for p in g], axis=0)
            tokens = flat(own)
            n = norm(tokens, gain[1, 0:1], shift[1, 0:1])
            n2 = norm(flat(beside), gain[1, 0:1], shift[1, 0:1])
            q, k, v = project(n, wfull, 2)
            r2 = dot_rows(n2, wfull[1:3].reshape(2 * C, C))
            k2 = (r2[:, 0:128] + bqkv[2, 1:2]).astype(BF)
            v2 = (r2[:, 128:256] + bqkv[2, 2:3]).astype(BF)
            attended = []
            for first_window in range(0, span, PACK):
                group = [min(first_window + i, span - 1) for i in range(PACK)]
                queries, keys, values, key_ids = [], [], [], []
                for g in group:
                    at = slice(32 * g, 32 * g + 32)
                    queries.append(jnp.concatenate([q[at] * m for m in heads], axis=0))
                    keys.append(jnp.concatenate([k[at], k2[at]], axis=0))
                    values.append(jnp.concatenate([v[at], v2[at]], axis=0))
                    key_ids += own_id[g] + beside_id[g]
                key_id = jnp.concatenate(key_ids, axis=0).T[0:8]
                width = 64 * len(group)
                allowed = [
                    jnp.concatenate([i[:, 0:width] == key_id for i in own_id[g]] * 4, axis=0)
                    for g in group
                ]
                for parts in weighted(queries, keys, values, bias1.at[1 - is_bottom], allowed, 32)[: span - first_window]:
                    mixed = parts[3]
                    for h in (2, 1, 0):
                        mixed = jnp.where(head_of == h, parts[h], mixed)
                    attended.append(mixed.astype(BF))
            done = feed(1, jnp.concatenate(attended, axis=0), tokens)
            for g in range(span):
                for r in range(SHIFT):
                    i = 32 * g + 8 * r
                    y[mine + r, pl.ds(base + WIN * g, WIN), :] = done[i : i + 8]
            return carry

        lax.fori_loop(0, SPANS, body, 0)
        row = SHIFT * is_bottom
        for r in range(SHIFT):
            out_ref[row + r] = y[mine + r, SHIFT : SHIFT + cols, :].astype(BF)

    shifted_band(1 - ch)
    shifted_band(ch)

    for c in first + second + third + side_regions + side_copies:
        c.wait_send()
    for k in range(chunks):
        for near in (True, False):
            halo_copy(near, k).wait_send()
    for near in (True, False):
        for c in corner_copies(near) + band_regions(near):
            c.wait_send()


def on_device(
    image_tokens, labels, rel_index, norm_gain, norm_shift, qkv_weight, qkv_bias, bias_table,
    proj_weight, proj_bias, fc1_weight, fc1_bias, fc2_weight, fc2_bias,
):
    rows, cols, _ = image_tokens.shape
    args = (
        image_tokens, labels, rel_index, norm_gain, norm_shift,
        jnp.swapaxes(qkv_weight, 2, 3), jnp.swapaxes(qkv_bias, 0, 1),
        jnp.swapaxes(bias_table, 1, 2),
        proj_weight, proj_bias, fc1_weight, fc1_bias, fc2_weight, fc2_bias,
    )
    V = pltpu.VMEM
    like = lambda a, *lead: V((*lead, *a.shape), a.dtype)
    copies = 34
    return pl.pallas_call(
        kernel,
        out_shape=pltpu.VMEM((rows, cols, C), BF),
        in_specs=[pl.BlockSpec(memory_space=pl.ANY)] * len(args),
        out_specs=pl.BlockSpec(memory_space=pltpu.VMEM),
        scratch_shapes=[
            like(image_tokens), like(labels), like(rel_index), like(norm_gain), like(norm_shift),
            like(args[6], 2), like(args[7], 2),
            V((2, C, C), BF), like(proj_bias),
            like(fc1_weight, 2), like(fc1_bias, 2), like(fc2_weight, 2), like(fc2_bias),
            V((3, C, C), BF), V((3, C, C), BF), V((3, C, C), BF),
            V((3, 3, C), F32),
            V((2, PACK, C, C), F32), V((2, PACK, C, C), F32),
            V((2 * WIN, cols + 8, C), F32), V((2 * WIN, cols + 8, C), F32),
            V((rows * cols, C), BF), V((rows * cols, C), BF),
            V((2, SHIFT, cols), jnp.int32), V((2, SHIFT, cols), jnp.int32),
            V((2, 2, SHIFT, 128), jnp.int32), V((4, SHIFT, 128), jnp.int32),
            V((rows, cols, C), BF), V((2, SHIFT, cols, C), BF),
            V((2, rows, 16, C), BF), V((4, SHIFT, 16, C), BF),
            pltpu.SemaphoreType.REGULAR,
            pltpu.SemaphoreType.DMA((15,)),
            pltpu.SemaphoreType.DMA((copies,)),
            pltpu.SemaphoreType.DMA((copies,)),
        ],
        compiler_params=pltpu.CompilerParams(
            collective_id=0, has_side_effects=True, vmem_limit_bytes=60 * 1024 * 1024
        ),
        name="swin_pair",
    )(*args)


def solution(mesh):
    in_specs = (
        P(("row", "ch"), "col", None),
        P(("row", "ch"), "col"),
        P(),
        P(),
        P(),
        P(None, None, None, "ch"),
        P(None, None, "ch"),
        P(None, None, "ch"),
        P(None, "ch", None),
        P(),
        P(None, None, "ch"),
        P(None, "ch"),
        P(None, "ch", None),
        P(),
    )
    out_specs = P(("row", "ch"), "col", None)
    return jax.shard_map(
        on_device, mesh=mesh, in_specs=in_specs, out_specs=out_specs, check_vma=False
    )
```

```python
import functools
import math

import jax
import jax.numpy as jnp
from jax import lax
from jax.experimental import pallas as pl
from jax.experimental.pallas import tpu as pltpu
from jax.sharding import PartitionSpec as P

WIN = 8
SHIFT = 4
HEADS = 4
EPS = 1e-05
C = 128
HEAD = 32
BF = jnp.bfloat16
F32 = jnp.float32
LOG2E = math.log2(math.e)
QSCALE = LOG2E / math.sqrt(HEAD)
ROOT_HALF = math.sqrt(0.5)
EXCLUDED = -1e30
MESH = pl.DeviceIdType.MESH

GROUP = 8
CHUNK = GROUP * WIN
PACK = 2
SPANS = 3


def norm(x, gain, shift):
    center = x - jnp.mean(x, axis=-1, keepdims=True)
    spread = jnp.mean(center * center, axis=-1, keepdims=True)
    return (center * lax.rsqrt(spread + EPS) * gain + shift).astype(BF)


def dot(a, b):
    return jnp.dot(a, b, preferred_element_type=F32)


def dot_rows(a, b):
    return lax.dot_general(a, b, (((1,), (1,)), ((), ())), preferred_element_type=F32)


def kernel(
    x_in, lab_in, rel_in, gain_in, shift_in, qkvw_in, qkvb_in, tbl_in, projw_in,
    projb_in, fc1w_in, fc1b_in, fc2w_in, fc2b_in,
    out_ref,
    x, lab, rel, gain, shift, qkvb, tbl, wproj, projb, w1, b1, w2, fc2b,
    wown, woth, wfull, bqkv, bias0, bias1,
    y, ids, normed, att, region, lab_row, lab_side, lab_corner,
    halo, both, patches, sides, corners,
    ready, local, send, recv,
):
    cols = x.shape[1]
    chunks = cols // CHUNK
    wins = cols // WIN + 1
    span = wins // SPANS
    groups = lax.axis_size("ch")
    bands = lax.axis_size("row") * groups
    tiles = lax.axis_size("col")
    ch = lax.axis_index("ch")
    col = lax.axis_index("col")
    band = lax.axis_index("row") * groups + ch

    def device(band_step, col_step):
        b = lax.rem(band + bands + band_step, bands)
        c = lax.rem(col + tiles + col_step, tiles)
        return {"row": b // groups, "col": c, "ch": lax.rem(b, groups)}

    partner = {"row": lax.axis_index("row"), "col": col, "ch": 1 - ch}
    across = {"row": lax.axis_index("row"), "col": lax.rem(col + tiles // 2, tiles), "ch": 1 - ch}
    up, down = device(-1, 0), device(1, 0)
    left, right = device(0, -1), device(0, 1)

    def towards(near):
        to_down = 1 - ch if near else ch
        return to_down, [device(2 * to_down - 1, side) for side in (0, -1, 1)]

    barrier = pltpu.get_barrier_semaphore()
    peers = [left, right, across] + towards(True)[1]
    strangers = towards(False)[1]

    def greet(semaphore, devices):
        for to in devices:
            pl.semaphore_signal(semaphore, inc=1, device_id=to, device_id_type=MESH)

    greet(barrier, peers)
    pl.when(ch == 0)(lambda: greet(barrier, strangers))

    def load(i, src, dst):
        return pltpu.make_async_copy(src, dst, local.at[i])

    own_rows = pl.ds(0, 64)
    other_rows = pl.ds(64, 64)
    early = [
        load(0, x_in, x),
        load(1, qkvw_in.at[0], wown.at[:, own_rows]),
        load(2, qkvb_in, qkvb.at[0]),
        load(3, tbl_in, tbl.at[0]),
        load(4, rel_in, rel),
        load(5, gain_in, gain),
        load(6, shift_in, shift),
    ]
    late = [
        load(7, projw_in, wproj.at[:, own_rows]),
        load(8, fc1w_in, w1.at[0]),
        load(9, fc1b_in, b1.at[0]),
        load(10, fc2w_in, w2.at[0]),
        load(11, qkvw_in.at[1], wfull.at[:, own_rows]),
        load(12, projb_in, projb),
        load(13, fc2b_in, fc2b),
        load(14, lab_in, lab),
    ]
    for c in early + late:
        c.start()

    wown[:, 64:128, :] = jnp.zeros((3, 64, C), BF)
    woth[:, 0:64, :] = jnp.zeros((3, 64, C), BF)

    def copy(i, src, dst, to):
        return pltpu.make_async_remote_copy(
            src_ref=src, dst_ref=dst, send_sem=send.at[i], recv_sem=recv.at[i],
            device_id=to, device_id_type=MESH,
        )

    first = [
        copy(0, wown.at[:, own_rows], woth.at[:, other_rows], partner),
        copy(1, qkvb.at[0], qkvb.at[1], partner),
        copy(2, tbl.at[0], tbl.at[1], partner),
        copy(3, b1.at[0], b1.at[1], partner),
    ]
    def feed_copies(b):
        return [
            copy(4 + 4 * b, wproj.at[b, own_rows], wproj.at[b, other_rows], across),
            copy(5 + 4 * b, w1.at[0, b], w1.at[1, b], (partner, across)[b]),
            copy(6 + 4 * b, w2.at[0, b], w2.at[1, b], across),
        ]
    second = feed_copies(0)
    third = [copy(7, wfull.at[:, own_rows], wfull.at[:, other_rows], across)] + feed_copies(1)
    half_at = {-1: pl.ds(0, 128), 1: pl.ds(cols - 128, 128)}
    side_regions = [
        copy(13, region.at[:, :, half_at[-1]], lab_side.at[1], left),
        copy(14, region.at[:, :, half_at[1]], lab_side.at[0], right),
    ]

    def band_regions(near):
        to_down, (to, *diagonals) = towards(near)
        return [copy(11 + to_down, region.at[to_down], lab_row.at[to_down], to)] + [
            copy(
                15 + 2 * to_down + i, region.at[to_down, :, half_at[side]],
                lab_corner.at[2 * to_down + i], diagonals[i],
            )
            for i, side in enumerate((-1, 1))
        ]

    for c in early:
        c.wait()

    lane = lax.broadcasted_iota(jnp.int32, (1, C), 1)
    head_of = lane // HEAD
    heads = [(head_of == h).astype(F32).astype(BF) for h in range(HEADS)]

    entries = tbl.shape[-1]

    def lookup(index, side, b, h):
        line = tbl[side, b, h : h + 1, :]
        a0 = jnp.broadcast_to(line[:, 0:128], index.shape)
        a1 = jnp.concatenate([line[:, 128:], jnp.zeros((1, 256 - entries), F32)], axis=1)
        a1 = jnp.broadcast_to(a1, index.shape)
        within = jnp.bitwise_and(index, 127)
        g0 = jnp.take_along_axis(a0, within, axis=1)
        g1 = jnp.take_along_axis(a1, within, axis=1)
        return jnp.where(index < 128, g0, g1) * LOG2E

    def put_bias(bias, i, rows, values):
        bias[i, 0, rows] = jnp.where(lane < 64, values, EXCLUDED)
        bias[i, 1, rows] = jnp.where(lane < 64, EXCLUDED, values)

    def first_bias(side):
        twice = jnp.concatenate([rel[...], rel[...]], axis=1)
        for h in range(2):
            put_bias(bias0, side, slice(64 * h, 64 * h + 64), lookup(twice, side, 0, h))

    def zero_padded(values, side):
        pad = jnp.zeros_like(values)
        return jnp.concatenate([values, pad] if side == 0 else [pad, values], axis=1)

    first_bias(0)
    for m in range(3):
        bqkv[0, m : m + 1] = zero_padded(qkvb[0, m, 0:1], 0)

    def project(n, w, b):
        r = dot_rows(n, w[...].reshape(3 * C, C))
        q = ((r[:, 0:128] + bqkv[b, 0:1]) * QSCALE).astype(BF)
        k = (r[:, 128:256] + bqkv[b, 1:2]).astype(BF)
        v = (r[:, 256:384] + bqkv[b, 2:3]).astype(BF)
        return q, k, v

    def weighted(queries, keys, values, bias, allowed, each):
        width = 64 * len(queries)
        s = dot_rows(jnp.concatenate(queries, axis=0), jnp.concatenate(keys, axis=0))
        s = [s[C * i : C * i + C] + bias[i, :, 0:width] for i in range(len(queries))]
        if allowed is not None:
            s = [jnp.where(a, b, EXCLUDED) for a, b in zip(allowed, s)]
        raised = [jnp.exp2(a - jnp.max(a, axis=1, keepdims=True)) for a in s]
        totals = [jnp.sum(a, axis=1, keepdims=True) for a in raised]
        o = dot(
            jnp.concatenate([a.astype(BF) for a in raised], axis=0),
            jnp.concatenate(values, axis=0),
        )
        mixed = []
        for i, total in enumerate(totals):
            part = o[C * i : C * i + C] * (1.0 / total)
            mixed.append([part[k : k + each] for k in range(0, C, each)])
        return mixed

    def half_attention(side, q, k, v):
        cut = lambda a: [a[64 * g : 64 * g + 64] for g in range(GROUP)]
        stacked = [
            jnp.concatenate([a * heads[2 * side], a * heads[2 * side + 1]], axis=0) for a in cut(q)
        ]
        k, v = cut(k), cut(v)
        out = []
        for g in range(0, GROUP, 2):
            two = slice(g, g + 2)
            for o0, o1 in weighted(stacked[two], k[two], v[two], bias0.at[side], None, 64):
                out.append(jnp.where(head_of == 2 * side, o0, o1).astype(BF))
        return jnp.concatenate(out, axis=0)

    def windows_of(base):
        lines = [x[r, pl.ds(base, CHUNK), :].astype(F32) for r in range(WIN)]
        return jnp.concatenate(
            [lines[r][WIN * g : WIN * g + WIN] for g in range(GROUP) for r in range(WIN)], axis=0
        )

    def meet():
        for c in late:
            c.wait()
        i = lax.broadcasted_iota(jnp.int32, lab.shape, 0)
        j = lax.broadcasted_iota(jnp.int32, lab.shape, 1)
        first_band = (band == 0).astype(jnp.int32)
        first_tile = (col == 0).astype(jnp.int32)
        regions = (
            lab[...] * 4
            + (i < SHIFT).astype(jnp.int32) * (2 * first_band)
            + (j < SHIFT).astype(jnp.int32) * first_tile
        )
        for half in range(2):
            region[half] = regions[SHIFT * half : SHIFT * half + SHIFT]

        pl.semaphore_wait(barrier, len(peers) + len(strangers) * ch)
        pl.when(ch == 1)(lambda: greet(ready, strangers))
        for c in first + second + third + side_regions + band_regions(True):
            c.start()

    def own_heads(j, carry):
        pl.when(j == 1)(meet)
        base = pl.multiple_of(j * CHUNK, CHUNK)
        at = pl.ds(pl.multiple_of(j * 64 * GROUP, 64 * GROUP), 64 * GROUP)
        n = norm(windows_of(base), gain[0, 0:1], shift[0, 0:1])
        normed[at, :] = n
        q, k, v = project(n, wown, 0)
        att[at, :] = half_attention(0, q, k, v)
        return carry

    lax.fori_loop(0, chunks, own_heads, 0)

    def spread(line):
        return jnp.broadcast_to(line.astype(F32), (128, 128)).T

    def put_middle(row, middle):
        for r in range(SHIFT):
            for t in range(cols // 128):
                ids[row + r, SHIFT + 128 * t : SHIFT + 128 * t + 128, :] = spread(
                    middle[r : r + 1, 128 * t : 128 * t + 128]
                )

    def put_ends(row, before, after):
        for r in range(SHIFT):
            line = slice(r, r + 1)
            ids[row + r, 0:SHIFT, :] = spread(before[line])[128 - SHIFT :]
            ids[row + r, SHIFT + cols : 2 * SHIFT + cols, :] = spread(after[line])[0:SHIFT]

    for half in range(2):
        put_middle(SHIFT + SHIFT * half, region.at[half])

    for c in first:
        c.wait_recv()
    first_bias(1)
    for m in range(3):
        bqkv[1, m : m + 1] = zero_padded(qkvb[1, m, 0:1], 1)
        bqkv[2, m : m + 1] = jnp.concatenate([qkvb[0, m, 1:2], qkvb[1, m, 1:2]], axis=1)
    for t, part in enumerate(
        (rel[0:32], jnp.concatenate([rel[32:64, 32:64], rel[32:64, 0:32]], axis=1))
    ):
        index = jnp.concatenate([part, part], axis=1)
        for h in range(HEADS):
            put_bias(bias1, t, slice(32 * h, 32 * h + 32), lookup(index, h // 2, 1, h % 2))

    def feed(b, attended, tokens):
        mid = (tokens + dot(attended, wproj[b]) + projb[b : b + 1]).astype(BF).astype(F32)
        n = norm(mid, gain[b, 1:2], shift[b, 1:2])
        total = mid + fc2b[b : b + 1]
        for side in range(2):
            inner = dot(n, w1[side, b]) + b1[side, b : b + 1]
            hidden = (inner * (0.5 + 0.5 * lax.erf(inner * ROOT_HALF))).astype(BF)
            total = total + dot(hidden, w2[side, b])
        return total.astype(BF).astype(F32)

    def halo_copy(near, k):
        at = pl.ds(pl.multiple_of(k * CHUNK, CHUNK), CHUNK)
        to_down = towards(near)[0]
        return copy(
            20 + 4 * to_down + k, halo.at[pl.ds(SHIFT * to_down, SHIFT), at],
            both.at[to_down, :, at], towards(near)[1][0],
        )

    side_copies = [
        copy(28, patches.at[0], sides.at[1], left),
        copy(29, patches.at[1], sides.at[0], right),
    ]

    def corner_copies(near):
        to_down, (_, *diagonals) = towards(near)
        return [
            copy(
                30 + 2 * to_down + i, patches.at[i, to_down],
                corners.at[2 * to_down + i], diagonals[i],
            )
            for i in range(2)
        ]

    def first_block(step, carry):
        k = lax.rem(step + chunks - 1, chunks)
        base = pl.multiple_of(k * CHUNK, CHUNK)
        at = pl.ds(pl.multiple_of(k * 64 * GROUP, 64 * GROUP), 64 * GROUP)
        q, key, v = project(normed[at, :], woth, 1)
        other = half_attention(1, q, key, v)

        @pl.when(step == 0)
        def _():
            for c in second:
                c.wait_recv()

        done = feed(0, att[at, :] + other, windows_of(base))
        for r in range(WIN):
            line = jnp.concatenate(
                [done[64 * g + 8 * r : 64 * g + 8 * r + 8] for g in range(GROUP)], axis=0
            )
            y[SHIFT + r, pl.ds(base + SHIFT, CHUNK), :] = line
            halo[r, pl.ds(base, CHUNK), :] = line.astype(BF)
        halo_copy(True, k).start()

        @pl.when(step == 1)
        def _():
            for e, at in enumerate((SHIFT, cols)):
                for half in range(2):
                    patches[e, half] = jnp.concatenate(
                        [y[SHIFT + SHIFT * half + r, at : at + SHIFT, :] for r in range(SHIFT)],
                        axis=0,
                    ).astype(BF)
            for c in side_copies + corner_copies(True):
                c.start()

        return carry

    lax.fori_loop(0, chunks, first_block, 0)

    pl.when(ch == 0)(lambda: pl.semaphore_wait(ready, len(strangers)))
    for c in band_regions(False) + corner_copies(False):
        c.start()
    for k in range(chunks):
        halo_copy(False, k).start()

    for c in side_regions:
        c.wait_recv()
    for half in range(2):
        put_ends(SHIFT + SHIFT * half, lab_side.at[0, half], lab_side.at[1, half])

    for c in third:
        c.wait_recv()
    for c in side_copies:
        c.wait_recv()
    ends = (slice(0, SHIFT), slice(SHIFT + cols, 2 * SHIFT + cols))

    def put_patch(row, to, patch):
        values = patch.astype(F32)
        for r in range(SHIFT):
            y[row + r, to, :] = values[SHIFT * r : SHIFT * r + SHIFT]

    for s, to in enumerate(ends):
        for half in range(2):
            put_patch(SHIFT + SHIFT * half, to, sides[s, half])

    def shifted_band(is_bottom):
        mine = SHIFT + SHIFT * is_bottom
        theirs = (SHIFT + WIN) * is_bottom

        arrived = both.at[1 - is_bottom]
        flow = 20 + 4 * (1 - is_bottom)

        def take(k):
            at = pl.ds(pl.multiple_of(k * CHUNK, CHUNK), CHUNK)
            copy(flow + k, arrived.at[:, at], arrived.at[:, at], up).wait_recv()
            for r in range(SHIFT):
                y[theirs + r, pl.ds(k * CHUNK + SHIFT, CHUNK), :] = arrived[r, at, :].astype(F32)

        above = 1 - is_bottom
        corner = 2 * above
        copy(11 + above, lab_row.at[above], lab_row.at[above], up).wait_recv()
        for i in range(2):
            part = lab_corner.at[corner + i]
            copy(15 + corner + i, part, part, up).wait_recv()
        put_middle(theirs, lab_row.at[above])
        put_ends(theirs, lab_corner.at[corner + 1], lab_corner.at[corner])
        for i in range(2):
            part = corners.at[corner + i]
            copy(30 + corner + i, part, part, up).wait_recv()
            put_patch(theirs, ends[1 - i], part[...])
        take(0)

        def body(c, carry):
            take(c + 1)
            base = pl.multiple_of(c * span * WIN, WIN)

            def gather(ref, row):
                return [
                    [ref[row + r, pl.ds(base + WIN * g, WIN), :] for r in range(SHIFT)]
                    for g in range(span)
                ]

            own = gather(y, mine)
            beside = gather(y, theirs)
            own_id = gather(ids, mine)
            beside_id = gather(ids, theirs)
            flat = lambda parts: jnp.concatenate([p for g in parts for p in g], axis=0)
            tokens = flat(own)
            n = norm(tokens, gain[1, 0:1], shift[1, 0:1])
            n2 = norm(flat(beside), gain[1, 0:1], shift[1, 0:1])
            q, k, v = project(n, wfull, 2)
            r2 = dot_rows(n2, wfull[1:3].reshape(2 * C, C))
            k2 = (r2[:, 0:128] + bqkv[2, 1:2]).astype(BF)
            v2 = (r2[:, 128:256] + bqkv[2, 2:3]).astype(BF)
            attended = []
            for first_window in range(0, span, PACK):
                group = [min(first_window + i, span - 1) for i in range(PACK)]
                queries, keys, values, key_ids = [], [], [], []
                for g in group:
                    at = slice(32 * g, 32 * g + 32)
                    queries.append(jnp.concatenate([q[at] * m for m in heads], axis=0))
                    keys.append(jnp.concatenate([k[at], k2[at]], axis=0))
                    values.append(jnp.concatenate([v[at], v2[at]], axis=0))
                    key_ids += own_id[g] + beside_id[g]
                key_id = jnp.concatenate(key_ids, axis=0).T[0:8]
                width = 64 * len(group)
                allowed = [
                    jnp.concatenate([i[:, 0:width] == key_id for i in own_id[g]] * 4, axis=0)
                    for g in group
                ]
                for parts in weighted(queries, keys, values, bias1.at[1 - is_bottom], allowed, 32)[: span - first_window]:
                    mixed = parts[3]
                    for h in (2, 1, 0):
                        mixed = jnp.where(head_of == h, parts[h], mixed)
                    attended.append(mixed.astype(BF))
            done = feed(1, jnp.concatenate(attended, axis=0), tokens)
            for g in range(span):
                for r in range(SHIFT):
                    i = 32 * g + 8 * r
                    y[mine + r, pl.ds(base + WIN * g, WIN), :] = done[i : i + 8]
            return carry

        lax.fori_loop(0, SPANS, body, 0)
        row = SHIFT * is_bottom
        for r in range(SHIFT):
            out_ref[row + r] = y[mine + r, SHIFT : SHIFT + cols, :].astype(BF)

    shifted_band(1 - ch)
    shifted_band(ch)

    for c in first + second + third + side_regions + side_copies:
        c.wait_send()
    for k in range(chunks):
        for near in (True, False):
            halo_copy(near, k).wait_send()
    for near in (True, False):
        for c in corner_copies(near) + band_regions(near):
            c.wait_send()


def on_device(
    image_tokens, labels, rel_index, norm_gain, norm_shift, qkv_weight, qkv_bias, bias_table,
    proj_weight, proj_bias, fc1_weight, fc1_bias, fc2_weight, fc2_bias,
):
    rows, cols, _ = image_tokens.shape
    args = (
        image_tokens, labels, rel_index, norm_gain, norm_shift,
        jnp.swapaxes(qkv_weight, 2, 3), jnp.swapaxes(qkv_bias, 0, 1),
        jnp.swapaxes(bias_table, 1, 2),
        proj_weight, proj_bias, fc1_weight, fc1_bias, fc2_weight, fc2_bias,
    )
    V = pltpu.VMEM
    like = lambda a, *lead: V((*lead, *a.shape), a.dtype)
    copies = 34
    return pl.pallas_call(
        kernel,
        out_shape=pltpu.VMEM((rows, cols, C), BF),
        in_specs=[pl.BlockSpec(memory_space=pl.ANY)] * len(args),
        out_specs=pl.BlockSpec(memory_space=pltpu.VMEM),
        scratch_shapes=[
            like(image_tokens), like(labels), like(rel_index), like(norm_gain), like(norm_shift),
            like(args[6], 2), like(args[7], 2),
            V((2, C, C), BF), like(proj_bias),
            like(fc1_weight, 2), like(fc1_bias, 2), like(fc2_weight, 2), like(fc2_bias),
            V((3, C, C), BF), V((3, C, C), BF), V((3, C, C), BF),
            V((3, 3, C), F32),
            V((2, PACK, C, C), F32), V((2, PACK, C, C), F32),
            V((2 * WIN, cols + 8, C), F32), V((2 * WIN, cols + 8, C), F32),
            V((rows * cols, C), BF), V((rows * cols, C), BF),
            V((2, SHIFT, cols), jnp.int32), V((2, SHIFT, cols), jnp.int32),
            V((2, 2, SHIFT, 128), jnp.int32), V((4, SHIFT, 128), jnp.int32),
            V((rows, cols, C), BF), V((2, SHIFT, cols, C), BF),
            V((2, 2, 16, C), BF), V((2, 2, 16, C), BF), V((4, 16, C), BF),
            pltpu.SemaphoreType.REGULAR,
            pltpu.SemaphoreType.DMA((15,)),
            pltpu.SemaphoreType.DMA((copies,)),
            pltpu.SemaphoreType.DMA((copies,)),
        ],
        compiler_params=pltpu.CompilerParams(
            collective_id=0, has_side_effects=True, vmem_limit_bytes=60 * 1024 * 1024
        ),
        name="swin_pair",
    )(*args)


def solution(mesh):
    in_specs = (
        P(("row", "ch"), "col", None),
        P(("row", "ch"), "col"),
        P(),
        P(),
        P(),
        P(None, None, None, "ch"),
        P(None, None, "ch"),
        P(None, None, "ch"),
        P(None, "ch", None),
        P(),
        P(None, None, "ch"),
        P(None, "ch"),
        P(None, "ch", None),
        P(),
    )
    out_specs = P(("row", "ch"), "col", None)
    return jax.shard_map(
        on_device, mesh=mesh, in_specs=in_specs, out_specs=out_specs, check_vma=False
    )
```
